256 devices in a mesh: level: 2 (over core), gx: 4 (over x), yz: 32 (over z, y).
Axes of the slice: x: 4, y: 4, z: 8, core: 2. Of those that a mesh axis runs over, the one named last changes fastest.
Arguments:
- init_field: float32 [128, 512, 256], P('gx', 'yz'), may hold values from -6 to 6
- source: float32 [128, 512, 256], P('gx', 'yz'), may hold values from -4 to 4
- damping: float32 [128, 512, 256], P('gx', 'yz'), may hold values from 0.05 to 2
Outputs:
- final_states: float32 [2, 128, 512, 256], P('level', 'gx', 'yz')
The draws below stay inside these ranges and needn't reach their ends.
All inputs are finite; a program needn't handle non-finite values.
Results may differ from the reference program's by a relative error of at most 0.0001.
Values sent between devices are 32-bit elements; how exact they have to be, the bound alone decides.
A program may use at most 64 MiB of HBM per device.

```python
import math
import jax
import jax.numpy as jnp

STEPS = 3
ITERS = 3
NX = 128
NY = 512
NZ = 256


def block_scale(rng, extent, split, low, high):
    level, own = 1.0, jax.random.fold_in(rng, 6)
    for position, parts in split:
        steps = jnp.exp(jax.random.uniform(jax.random.fold_in(own, position), (parts,), jnp.float32, low / len(split), high / len(split)))
        level = level * jnp.repeat(steps, extent[position] // parts).reshape([-1 if axis == position else 1 for axis in range(len(extent))])
    return level


def noise(stream_key, shape, deviation, most, shards=(), dtype=jnp.bfloat16):
    gain = block_scale(stream_key, shape, shards, -0.22, 0.18) if shards else 1.0
    array = jax.random.normal(stream_key, shape, jnp.float32) * deviation * gain
    return jnp.minimum(jnp.maximum(array, -most), most).astype(dtype)


def setup_inputs(seed: int = 0) -> dict:
    keys = jax.random.split(jax.random.key(seed), 4)
    init_field = noise(keys[0], (NX, NY, NZ), 1.0, 6.0, ((0, 4), (1, 32)), jnp.float32)
    source = noise(keys[1], (NX, NY, NZ), 0.5, 4.0, ((0, 4), (1, 32)), jnp.float32)
    damping = jnp.clip(jnp.exp(math.log(2.0) - 3.6888794 * jax.random.uniform(keys[2], (NX, NY, NZ), jnp.float32) ** block_scale(keys[2], (NX, NY, NZ), ((0, 4), (1, 32)), -0.2, 0.2)), 0.05, 2.0)
    return dict(init_field=init_field, source=source, damping=damping)


diffusion_number = 1.0


def stencil(field, damping):
    padded = jnp.pad(field, 1)
    beside = padded[2:, 1:-1, 1:-1] + padded[:-2, 1:-1, 1:-1]
    beside = beside + padded[1:-1, 2:, 1:-1] + padded[1:-1, :-2, 1:-1]
    beside = beside + padded[1:-1, 1:-1, 2:] + padded[1:-1, 1:-1, :-2]
    return damping * field + diffusion_number * (6.0 * field - beside)


def solve(target, guess, damping):
    answer = guess
    resid = target - (answer + stencil(answer, damping))
    direction = resid
    norm_now = jnp.sum(resid * resid)
    for step in range(ITERS):
        image = direction + stencil(direction, damping)
        alpha = norm_now / jnp.sum(direction * image)
        answer = answer + alpha * direction
        resid = resid - alpha * image
        if step + 1 < ITERS:
            norm_next = jnp.sum(resid * resid)
            direction = resid + (norm_next / norm_now) * direction
            norm_now = norm_next
    return answer


def reference(init_field, source, damping):
    states = [init_field]
    for step in range(STEPS):
        states.append(solve(states[-1] + source, states[-1], damping))
    corrected = init_field
    for step in range(STEPS):
        extra = 0.5 * stencil(states[step + 1] - states[step], damping)
        corrected = solve(corrected + source + extra, corrected, damping)
    return jnp.stack([states[-1], corrected])
```

```python
import functools

import jax
import jax.numpy as jnp
from jax import lax
from jax.experimental import pallas as pl
from jax.experimental.pallas import tpu as pltpu
from jax.sharding import PartitionSpec as P

STEPS = 3
ITERS = 3
ROUNDS = (3, 5)
PX = 4
PY = 8
LANES = 128
MID = 8.025
HALF = 6.975
MESH = pl.DeviceIdType.MESH
DIRS = ((-1, 0), (1, 0), (0, -1), (0, 1), (-1, -1), (-1, 1), (1, -1), (1, 1))


def times_a(c):
    out = [MID * v for v in c] + [jnp.zeros_like(c[0])]
    for k, v in enumerate(c):
        if k == 0:
            out[1] = out[1] + HALF * v
        else:
            out[k + 1] = out[k + 1] + (0.5 * HALF) * v
            out[k - 1] = out[k - 1] + (0.5 * HALF) * v
    return out


def plus(a, b):
    short, long = (a, b) if len(a) < len(b) else (b, a)
    return [x + y for x, y in zip(short, long)] + long[len(short):]


def scaled(s, a):
    return [s * x for x in a]


def cg_coefficients(dots):
    m = [dots[0], dots[1], 2.0 * dots[2] - dots[0], 2.0 * dots[3] - dots[1],
         2.0 * dots[4] - dots[0], 2.0 * dots[5] - dots[1]]

    def inner(a, b):
        total = None
        for i, x in enumerate(a):
            for j, y in enumerate(b):
                term = (x * y) * (0.5 * (m[i + j] + m[abs(i - j)]))
                total = term if total is None else total + term
        return total

    one = jnp.ones_like(m[0])
    resid = [one]
    direction = resid
    image = times_a(resid)
    along = image
    norm_now = m[0]
    alpha = norm_now / inner(resid, image)
    answer = None
    for step in range(ITERS):
        move = scaled(alpha, direction)
        answer = move if answer is None else plus(answer, move)
        if step + 1 < ITERS:
            resid = plus(resid, scaled(-alpha, along))
            image = times_a(resid)
            norm_next = inner(resid, resid)
            product = inner(resid, image)
            ratio = norm_next / norm_now
            alpha = norm_next / (product - ratio * norm_next / alpha)
            direction = plus(resid, scaled(ratio, direction))
            along = plus(image, scaled(ratio, along))
            norm_now = norm_next
    change = plus(times_a(answer), scaled(-1.0, answer))
    return answer, change


def shifted(change):
    table = []
    for j in range(ITERS + 1):
        row = [None] * (2 * ITERS + 1)
        for i, c in enumerate(change):
            for l in (i + j, abs(i - j)):
                row[l] = 0.5 * c if row[l] is None else row[l] + 0.5 * c
        for l in range(1, ITERS + 1):
            far = row[ITERS + l]
            if far is not None:
                near = row[ITERS - l]
                row[ITERS - l] = -far if near is None else near - far
                row[ITERS + l] = 2.0 * far
        table.append(row)
    return table


def combine(c, v):
    total = None
    for a, b in zip(c, v):
        if a is not None:
            total = a * b if total is None else total + a * b
    return total


def body(sizes, stages, init_ref, source_ref, damp_ref, out_ref, p0, src, dmp, first, heads_p, heads_c, own_p, own_c,
         base, work_p, work_c, sums, result, slots, in_sem, send_sem, recv_sem, red_send, red_recv, out_sem, p_send, p_recv,
         meet_x, meet_y):
    levels, nx, ny = sizes
    half = own_p.shape[1]
    parts = p0.shape[1]
    rows = own_p.shape[3]
    level, gx, yz = lax.axis_index("level"), lax.axis_index("gx"), lax.axis_index("yz")
    xpos = gx * levels + level
    xcount = nx * levels
    x_in = (xpos > 0, xpos < xcount - 1)
    y_in = (yz > 0, yz < ny - 1)

    def exists(dx, dy):
        ok = None
        for d, at, count in ((dx, xpos, xcount), (dy, yz, ny)):
            if d != 0:
                c = at + d >= 0 if d < 0 else at + d < count
                ok = c if ok is None else jnp.logical_and(ok, c)
        return ok

    def beside(dx, dy):
        to = xpos + dx
        return {"level": lax.rem(to + xcount, levels), "gx": lax.div(to + xcount, levels) - nx, "yz": yz + dy}

    mine = pl.ds(level * half, half)
    loads = []
    for i, (ref, buf) in enumerate(((init_ref, p0), (source_ref, src), (damp_ref, dmp))):
        for z in range(parts):
            copy = pltpu.make_async_copy(ref.at[mine, :, slice(z * LANES, (z + 1) * LANES)],
                                         buf.at[PX:PX + half, z, PY:PY + rows, :], in_sem.at[i, z])
            copy.start()
            loads.append(copy)

    def signal_all(sem, steps):
        count = 0
        for dx, dy in steps:
            ok = exists(dx, dy)
            count = count + jnp.where(ok, 1, 0)

            @pl.when(ok)
            def _(dx=dx, dy=dy):
                pl.semaphore_signal(sem, inc=1, device_id=beside(dx, dy), device_id_type=MESH)
        return count

    def meet(turn):
        if turn > 0:
            for sem, rounds, axis in ((meet_x, ROUNDS[0], 0), (meet_y, ROUNDS[1], 1)):
                if turn <= rounds:
                    far = 2 ** (turn - 1)
                    count = 0
                    for d in (-far, far):
                        count = count + jnp.where(exists(*((d, 0) if axis == 0 else (0, d))), 1, 0)
                    pl.semaphore_wait(sem.at[turn - 1], count)
        for sem, rounds, axis in ((meet_x, ROUNDS[0], 0), (meet_y, ROUNDS[1], 1)):
            if turn < rounds:
                far = 2 ** turn
                signal_all(sem.at[turn], [(d, 0) if axis == 0 else (0, d) for d in (-far, far)])

    barrier = pltpu.get_barrier_semaphore()
    greeted = signal_all(barrier, DIRS)

    zero_x = jnp.zeros((PX,) + tuple(p0.shape[1:]), jnp.float32)
    zero_y = jnp.zeros((p0.shape[0], parts, PY, LANES), jnp.float32)
    for buf in [p0] + [heads_p.at[n] for n in range(STEPS)] + [heads_c.at[n] for n in range(STEPS - 1)]:
        @pl.when(jnp.logical_not(x_in[0]))
        def _(buf=buf):
            buf[0:PX] = zero_x

        @pl.when(jnp.logical_not(x_in[1]))
        def _(buf=buf):
            buf[PX + half:] = zero_x

        @pl.when(jnp.logical_not(y_in[0]))
        def _(buf=buf):
            buf[:, :, 0:PY, :] = zero_y

        @pl.when(jnp.logical_not(y_in[1]))
        def _(buf=buf):
            buf[:, :, PY + rows:, :] = zero_y

    def halo_copy(buf, width, slot, k):
        dx, dy = DIRS[k]
        w = width if 0 in (dx, dy) else width - 1

        def spans(d, pad, size):
            if d == 0:
                return slice(pad, pad + size), slice(pad, pad + size)
            if d < 0:
                return slice(pad, pad + w), slice(pad + size, pad + size + w)
            return slice(pad + size - w, pad + size), slice(pad - w, pad)

        sx, tx = spans(dx, PX, half)
        sy, ty = spans(dy, PY, rows)
        return pltpu.make_async_remote_copy(
            src_ref=buf.at[sx, :, sy, :], dst_ref=buf.at[tx, :, ty, :],
            send_sem=send_sem.at[slot, k], recv_sem=recv_sem.at[slot, k],
            device_id=beside(dx, dy), device_id_type=MESH,
        )

    order = (2, 3, 4, 5, 6, 7, 0, 1)

    def send_halo(*item):
        for k in order:
            pl.when(exists(*DIRS[k]))(lambda k=k: halo_copy(*item, k).start())

    def wait_halo(*item):
        for k in order:
            dx, dy = DIRS[k]
            pl.when(exists(-dx, -dy))(lambda k=k: halo_copy(*item, k).wait_recv())

    def end_halo(*item):
        for k in order:
            pl.when(exists(*DIRS[k]))(lambda k=k: halo_copy(*item, k).wait_send())

    def stencil(v, x, start, count):
        lane = lax.broadcasted_iota(jnp.int32, (count, LANES), 1)
        own = pl.ds(start, count)
        centre = [v[x, z, own, :] for z in range(parts)]
        fore = [pltpu.roll(c, 1, 1) for c in centre]
        back = [pltpu.roll(c, LANES - 1, 1) for c in centre]
        out = []
        for z in range(parts):
            near = jnp.where(lane == 0, fore[z - 1] if z > 0 else 0.0, fore[z])
            far = jnp.where(lane == LANES - 1, back[z + 1] if z + 1 < parts else 0.0, back[z])
            beside = v[x - 1, z, own, :] + v[x + 1, z, own, :]
            beside = beside + v[x, z, pl.ds(start - 1, count), :] + v[x, z, pl.ds(start + 1, count), :]
            beside = beside + (near + far)
            out.append((dmp[x, z, own, :] + (7.0 - MID)) * centre[z] - beside)
        return out, centre

    low = jnp.where(y_in[0], 0, PY)
    high = jnp.where(y_in[1], 2 * PY + rows, PY + rows)

    def fold(block):
        return jnp.sum(block.reshape(-1, 8, LANES), axis=0)

    def reach(h):
        return PY - h, -(-(rows + 2 * h) // 8) * 8

    def inside(x, start, count):
        row = lax.broadcasted_iota(jnp.int32, (count, LANES), 0) + start
        ok = jnp.logical_and(row >= low, row < high)
        if PX <= x < PX + half:
            return ok
        return jnp.logical_and(ok, x_in[0] if x < PX else x_in[1])

    def powers(head, work, with_dots=False, between=None):
        zero = jnp.zeros((8, LANES), jnp.float32)
        totals = []
        for k in range(1, ITERS + 1):
            h = ITERS - k
            start, count = reach(h)
            prev = head if k == 1 else work[k - 2]
            older = None if k == 1 else head if k == 2 else work[k - 3]
            row = lax.broadcasted_iota(jnp.int32, (count, LANES), 0) + start
            keep = jnp.logical_and(row >= PY, row < PY + rows)
            a, b = zero, zero
            for x in range(PX - h, PX + half + h):
                t, centre = stencil(prev, x, start, count)
                ok = inside(x, start, count)
                for z in range(parts):
                    if k == 1:
                        new = t[z] * (1.0 / HALF)
                    else:
                        new = t[z] * (2.0 / HALF) - older[x, z, pl.ds(start, count), :]
                    if h > 0:
                        new = jnp.where(ok, new, 0.0)
                    work[k - 1][x, z, pl.ds(start, count), :] = new
                    if with_dots and PX <= x < PX + half:
                        square, cross = centre[z] * centre[z], centre[z] * new
                        if h > 0:
                            square, cross = jnp.where(keep, square, 0.0), jnp.where(keep, cross, 0.0)
                        a = a + fold(square)
                        b = b + fold(cross)
            totals += [a, b]
            if between is not None:
                between(k)
        return totals

    def position(axes):
        flat = 0
        for a in axes:
            flat = flat * lax.axis_size(a) + lax.axis_index(a)
        return flat

    def reduce_all(accs, turn, outgoing, meanwhile):
        n = len(accs)
        size = -(-n // 8) * 8
        eye = lax.broadcasted_iota(jnp.int32, (size, LANES), 0) == lax.broadcasted_iota(jnp.int32, (size, LANES), 1)
        tall = jnp.concatenate([jnp.sum(a, axis=0, keepdims=True) for a in accs]
                               + [jnp.zeros((size - n, LANES), jnp.float32)] * (size > n), axis=0)
        col = jnp.sum(tall, axis=1, keepdims=True)
        line = jnp.sum(jnp.where(eye, col, 0.0), axis=0, keepdims=True)
        for s, axes in enumerate(stages):
            count = 1
            for a in axes:
                count *= lax.axis_size(a)
            me = position(axes)
            cell = slots[s].at[turn, pl.ds(me, 1), :]
            cell[...] = line
            copies = []
            for off in range(1, count):
                peer = lax.rem(me + off, count)
                ids = {}
                for a in reversed(axes):
                    ids[a] = lax.rem(peer, lax.axis_size(a))
                    peer = lax.div(peer, lax.axis_size(a))
                copy = pltpu.make_async_remote_copy(
                    src_ref=cell, dst_ref=cell, send_sem=red_send[s].at[turn, off - 1],
                    recv_sem=red_recv[s].at[turn, off - 1], device_id=ids, device_id_type=MESH)
                copy.start()
                copies.append(copy)
            if s == 0:
                for item in outgoing:
                    send_halo(*item)
            if s == len(stages) - 1:
                meanwhile()
            for copy in copies:
                copy.wait_recv()
            line = jnp.sum(slots[s][turn], axis=0, keepdims=True)
            for copy in copies:
                copy.wait_send()
            if s == 0 and turn == 0:
                meet(5)
        col = jnp.sum(jnp.where(eye, line, 0.0), axis=1, keepdims=True)
        wide = jnp.broadcast_to(col, (size, LANES))
        return [jnp.broadcast_to(wide[k:k + 1, :], (8, LANES)) for k in range(n)]

    def place(ref, f, part, z):
        return ref.at[0, pl.ds(part * half, half), :, slice(z * LANES, (z + 1) * LANES)]

    def piece(f, z):
        return pltpu.make_async_copy(result.at[f, :, z], place(out_ref, f, level, z), out_sem.at[z])

    def across(f, z):
        return pltpu.make_async_remote_copy(
            src_ref=result.at[f, :, z], dst_ref=place(out_ref, f, level, z), send_sem=p_send.at[z], recv_sem=p_recv.at[z],
            device_id={"level": f, "gx": gx, "yz": yz}, device_id_type=MESH)

    def deliver(f):
        for z in range(parts):
            pl.when(level != f)(lambda z=z: across(f, z).start())
            pl.when(level == f)(lambda z=z: piece(f, z).start())

    pl.semaphore_wait(barrier, greeted)
    meet(0)
    starts = ((p0, PX, 0), (dmp, PX - 1, 1), (src, PX - 1, 2))
    for item, at in zip(starts, (0, 2, 1)):
        for copy in loads[at * parts:(at + 1) * parts]:
            copy.wait()
        send_halo(*item)
    for item in starts:
        wait_halo(*item)
    meet(1)

    start, count = reach(ITERS)
    for x in range(PX - ITERS, PX + half + ITERS):
        t, centre = stencil(p0, x, start, count)
        ok = inside(x, start, count)
        for z in range(parts):
            r = src[x, z, pl.ds(start, count), :] - (t[z] + (MID - 1.0) * centre[z])
            first[0, x, z, pl.ds(start, count), :] = jnp.where(ok, r, 0.0)
    meet(2)
    accs = powers(first.at[0], (first.at[1], first.at[2], heads_p.at[0]), True,
                  lambda k: meet(k + 2) if k < ITERS else None)

    pending = list(starts)
    slot = len(starts)
    for turn in range(STEPS + 1):
        with_p, with_c = turn < STEPS, turn > 0
        outgoing, jobs = [], []
        if with_p:
            outgoing.append((heads_p.at[turn], ITERS, slot))
            jobs.append((heads_p.at[turn], work_p))
            slot += 1
        if with_p and with_c:
            outgoing.append((heads_c.at[turn - 1], ITERS, slot))
            jobs.append((heads_c.at[turn - 1], work_c))
            slot += 1

        def meanwhile(outgoing=outgoing, jobs=jobs):
            for item, (head, work) in zip(outgoing, jobs):
                wait_halo(*item)
                powers(head, [work.at[k] for k in range(ITERS)])

        pending += outgoing
        dots = reduce_all(accs, turn, outgoing, meanwhile)
        sets = [cg_coefficients(dots[6 * i:6 * i + 6]) for i in range(len(dots) // 6)]
        if with_p:
            rise_p, table_p = sets[0][0], shifted(sets[0][1])
        if with_c:
            rise_c, table_c = sets[-1][0], shifted(sets[-1][1])
        n_acc = 6 * ((turn + 1 < STEPS) + (turn < STEPS))

        def update(i, accs):
            x = i + PX
            accs = list(accs)
            for z in range(parts):
                for y in range(0, rows, 8):
                    near, wide = pl.ds(y, 8), pl.ds(PY + y, 8)
                    if with_p:
                        if turn == 0:
                            v = [first[j, x, z, wide, :] for j in range(ITERS)]
                        else:
                            v = [own_p[j, i, z, near, :] for j in range(ITERS)]
                        v.append(heads_p[turn, x, z, wide, :])
                        v += [work_p[k, x, z, wide, :] for k in range(ITERS)]
                        before = p0[x, z, wide, :] if turn == 0 else sums[0, i, z, near, :]
                        after = before + combine(rise_p, v)
                        if turn + 1 < STEPS:
                            sums[0, i, z, near, :] = after
                        else:
                            result[0, i, z, near, :] = after
                        change = [combine(row, v) for row in table_p]
                    if with_c:
                        u = [own_c[j, i, z, near, :] for j in range(ITERS)]
                        before = p0[x, z, wide, :] if turn == 1 else sums[1, i, z, near, :]
                        after = before + combine(rise_c, u)
                        if turn < STEPS:
                            sums[1, i, z, near, :] = after
                            u.append(heads_c[turn - 1, x, z, wide, :])
                            u += [work_c[k, x, z, wide, :] for k in range(ITERS)]
                        else:
                            result[1, i, z, near, :] = after
                    if turn == STEPS:
                        continue
                    news = []
                    if turn + 1 < STEPS:
                        fresh = [a - b for a, b in zip(v, change)]
                        for j in range(ITERS):
                            own_p[j, i, z, near, :] = fresh[j]
                        heads_p[turn + 1, x, z, wide, :] = fresh[ITERS]
                        news.append(fresh)
                    if turn == 0:
                        ground = v[:ITERS + 1]
                    else:
                        if turn == 1:
                            ground = [first[j, x, z, wide, :] for j in range(ITERS)] + [heads_p[0, x, z, wide, :]]
                        else:
                            ground = [base[j, i, z, near, :] for j in range(ITERS + 1)]
                        ground = [a - combine(row, u) for a, row in zip(ground, table_c)]
                        if turn + 1 < STEPS:
                            for j in range(ITERS + 1):
                                base[j, i, z, near, :] = ground[j]
                    fresh = [a + 0.5 * b for a, b in zip(ground, change)]
                    for j in range(ITERS):
                        own_c[j, i, z, near, :] = fresh[j]
                    heads_c[turn, x, z, wide, :] = fresh[ITERS]
                    news.append(fresh)
                    for f, fresh in enumerate(news):
                        for j in range(ITERS):
                            accs[6 * f + 2 * j] = accs[6 * f + 2 * j] + fresh[j] * fresh[j]
                            accs[6 * f + 2 * j + 1] = accs[6 * f + 2 * j + 1] + fresh[j] * fresh[j + 1]
            return tuple(accs)

        accs = lax.fori_loop(0, half, update, (jnp.zeros((8, LANES), jnp.float32),) * n_acc)
        if turn == STEPS - 1:
            deliver(0)
    deliver(1)
    for item in pending:
        end_halo(*item)
    for f in range(2):
        for z in range(parts):
            pl.when(level != f)(lambda f=f, z=z: across(f, z).wait_send())
            pl.when(level == f)(lambda f=f, z=z: across(f, z).wait_recv())
            pl.when(level == f)(lambda f=f, z=z: piece(f, z).wait())


def solution(mesh):
    levels, nx, ny = mesh.shape["level"], mesh.shape["gx"], mesh.shape["yz"]
    stages = (("level", "gx"), ("yz",))

    def per_device(init_field, source, damping):
        deep, rows, wide = init_field.shape
        half, parts = deep // levels, wide // LANES
        padded = (half + 2 * PX, parts, rows + 2 * PY, LANES)
        plain = (half, parts, rows, LANES)
        counts = []
        for axes in stages:
            n = 1
            for a in axes:
                n *= mesh.shape[a]
            counts.append(n)
        turns = STEPS + 1
        dma = pltpu.SemaphoreType.DMA
        exchanges = 3 + 2 * STEPS - 1
        vmem = lambda n, shape: pltpu.VMEM((n,) + shape, jnp.float32)
        return pl.pallas_call(
            functools.partial(body, (levels, nx, ny), stages),
            out_shape=jax.ShapeDtypeStruct((1, deep, rows, wide), jnp.float32),
            in_specs=[pl.BlockSpec(memory_space=pl.ANY)] * 3,
            out_specs=pl.BlockSpec(memory_space=pl.ANY),
            scratch_shapes=[
                pltpu.VMEM(padded, jnp.float32),
                pltpu.VMEM(padded, jnp.float32),
                pltpu.VMEM(padded, jnp.float32),
                vmem(ITERS, padded),
                vmem(STEPS, padded),
                vmem(STEPS, padded),
                vmem(ITERS, plain),
                vmem(ITERS, plain),
                vmem(ITERS + 1, plain),
                vmem(ITERS, padded),
                vmem(ITERS, padded),
                vmem(2, plain),
                vmem(2, plain),
                [pltpu.VMEM((turns, n, LANES), jnp.float32) for n in counts],
                dma((3, parts)),
                dma((exchanges, 8)),
                dma((exchanges, 8)),
                [dma((turns, n - 1)) for n in counts],
                [dma((turns, n - 1)) for n in counts],
                dma((parts,)),
                dma((parts,)),
                dma((parts,)),
                pltpu.SemaphoreType.REGULAR((ROUNDS[0],)),
                pltpu.SemaphoreType.REGULAR((ROUNDS[1],)),
            ],
            compiler_params=pltpu.CompilerParams(has_side_effects=True, collective_id=0),
        )(init_field, source, damping)

    spec = P("gx", "yz", None)
    return jax.shard_map(
        per_device, mesh=mesh, in_specs=(spec, spec, spec),
        out_specs=P("level", "gx", "yz", None), check_vma=False,
    )
```

```python
import functools

import jax
import jax.numpy as jnp
from jax import lax
from jax.experimental import pallas as pl
from jax.experimental.pallas import tpu as pltpu
from jax.sharding import PartitionSpec as P

STEPS = 3
ITERS = 3
ROUNDS = 5
INNER = 4
PX = 4
PY = 8
LANES = 128
MID = 8.025
HALF = 6.975
MESH = pl.DeviceIdType.MESH
DIRS = ((-1, 0), (1, 0), (0, -1), (0, 1), (-1, -1), (-1, 1), (1, -1), (1, 1))


def times_a(c):
    out = [MID * v for v in c] + [jnp.zeros_like(c[0])]
    for k, v in enumerate(c):
        if k == 0:
            out[1] = out[1] + HALF * v
        else:
            out[k + 1] = out[k + 1] + (0.5 * HALF) * v
            out[k - 1] = out[k - 1] + (0.5 * HALF) * v
    return out


def plus(a, b):
    short, long = (a, b) if len(a) < len(b) else (b, a)
    return [x + y for x, y in zip(short, long)] + long[len(short):]


def scaled(s, a):
    return [s * x for x in a]


def cg_coefficients(dots):
    m = [dots[0], dots[1], 2.0 * dots[2] - dots[0], 2.0 * dots[3] - dots[1],
         2.0 * dots[4] - dots[0], 2.0 * dots[5] - dots[1]]

    def inner(a, b):
        total = None
        for i, x in enumerate(a):
            for j, y in enumerate(b):
                term = (x * y) * (0.5 * (m[i + j] + m[abs(i - j)]))
                total = term if total is None else total + term
        return total

    one = jnp.ones_like(m[0])
    resid = [one]
    direction = resid
    image = times_a(resid)
    along = image
    norm_now = m[0]
    alpha = norm_now / inner(resid, image)
    answer = None
    for step in range(ITERS):
        move = scaled(alpha, direction)
        answer = move if answer is None else plus(answer, move)
        if step + 1 < ITERS:
            resid = plus(resid, scaled(-alpha, along))
            image = times_a(resid)
            norm_next = inner(resid, resid)
            product = inner(resid, image)
            ratio = norm_next / norm_now
            alpha = norm_next / (product - ratio * norm_next / alpha)
            direction = plus(resid, scaled(ratio, direction))
            along = plus(image, scaled(ratio, along))
            norm_now = norm_next
    change = plus(times_a(answer), scaled(-1.0, answer))
    return answer, change


def shifted(change):
    table = []
    for j in range(ITERS + 1):
        row = [None] * (2 * ITERS + 1)
        for i, c in enumerate(change):
            for l in (i + j, abs(i - j)):
                row[l] = 0.5 * c if row[l] is None else row[l] + 0.5 * c
        for l in range(1, ITERS + 1):
            far = row[ITERS + l]
            if far is not None:
                near = row[ITERS - l]
                row[ITERS - l] = -far if near is None else near - far
                row[ITERS + l] = 2.0 * far
        table.append(row)
    return table


def combine(c, v):
    total = None
    for a, b in zip(c, v):
        if a is not None:
            total = a * b if total is None else total + a * b
    return total


def body(sizes, init_ref, source_ref, damp_ref, out_ref, p0, src, dmp, first, heads_p, heads_c, own_p, own_c,
         base, work_p, work_c, sums, result, slots, in_sem, send_sem, recv_sem, red_send, red_recv, p_send, p_recv,
         met):
    levels, nx, ny = sizes
    half = own_p.shape[1]
    parts = p0.shape[1]
    rows = own_p.shape[3]
    level, gx, yz = lax.axis_index("level"), lax.axis_index("gx"), lax.axis_index("yz")
    xpos = gx * levels + level
    xcount = nx * levels
    x_in = (xpos > 0, xpos < xcount - 1)
    y_in = (yz > 0, yz < ny - 1)

    def exists(dx, dy):
        ok = None
        for d, at, count in ((dx, xpos, xcount), (dy, yz, ny)):
            if d != 0:
                c = at + d >= 0 if d < 0 else at + d < count
                ok = c if ok is None else jnp.logical_and(ok, c)
        return ok

    def beside(dx, dy):
        to = xpos + dx
        return {"level": lax.rem(to + xcount, levels), "gx": lax.div(to + xcount, levels) - nx, "yz": yz + dy}

    mine = pl.ds(level * half, half)
    loads = []
    for i, (ref, buf) in enumerate(((init_ref, p0), (source_ref, src), (damp_ref, dmp))):
        for z in range(parts):
            copy = pltpu.make_async_copy(ref.at[mine, :, slice(z * LANES, (z + 1) * LANES)],
                                         buf.at[PX:PX + half, z, PY:PY + rows, :], in_sem.at[i, z])
            copy.start()
            loads.append(copy)

    def signal_all(sem, steps):
        count = 0
        for dx, dy in steps:
            ok = exists(dx, dy)
            count = count + jnp.where(ok, 1, 0)

            @pl.when(ok)
            def _(dx=dx, dy=dy):
                pl.semaphore_signal(sem, inc=1, device_id=beside(dx, dy), device_id_type=MESH)
        return count

    def meet(turn):
        if turn > 0:
            far = 2 ** (turn - 1)
            count = 0
            for d in (-far, far):
                count = count + jnp.where(exists(0, d), 1, 0)
            pl.semaphore_wait(met.at[turn - 1], count)
        if turn < ROUNDS:
            signal_all(met.at[turn], [(0, -2 ** turn), (0, 2 ** turn)])

    barrier = pltpu.get_barrier_semaphore()
    greeted = signal_all(barrier, DIRS + tuple((d, 0) for d in range(1 - xcount, xcount) if abs(d) > 1))

    zero_x = jnp.zeros((PX,) + tuple(p0.shape[1:]), jnp.float32)
    zero_y = jnp.zeros((p0.shape[0], parts, PY, LANES), jnp.float32)
    for buf in [p0] + [heads_p.at[n] for n in range(STEPS)] + [heads_c.at[n] for n in range(STEPS - 1)]:
        @pl.when(jnp.logical_not(x_in[0]))
        def _(buf=buf):
            buf[0:PX] = zero_x

        @pl.when(jnp.logical_not(x_in[1]))
        def _(buf=buf):
            buf[PX + half:] = zero_x

        @pl.when(jnp.logical_not(y_in[0]))
        def _(buf=buf):
            buf[:, :, 0:PY, :] = zero_y

        @pl.when(jnp.logical_not(y_in[1]))
        def _(buf=buf):
            buf[:, :, PY + rows:, :] = zero_y

    def halo_copy(buf, width, slot, k):
        dx, dy = DIRS[k]
        w = width if 0 in (dx, dy) else width - 1

        def spans(d, pad, size):
            if d == 0:
                return slice(pad, pad + size), slice(pad, pad + size)
            if d < 0:
                return slice(pad, pad + w), slice(pad + size, pad + size + w)
            return slice(pad + size - w, pad + size), slice(pad - w, pad)

        sx, tx = spans(dx, PX, half)
        sy, ty = spans(dy, PY, rows)
        return pltpu.make_async_remote_copy(
            src_ref=buf.at[sx, :, sy, :], dst_ref=buf.at[tx, :, ty, :],
            send_sem=send_sem.at[slot, k], recv_sem=recv_sem.at[slot, k],
            device_id=beside(dx, dy), device_id_type=MESH,
        )

    order = (2, 3, 4, 5, 6, 7, 0, 1)

    def send_halo(*item):
        for k in order:
            pl.when(exists(*DIRS[k]))(lambda k=k: halo_copy(*item, k).start())

    def wait_halo(*item):
        for k in order:
            dx, dy = DIRS[k]
            pl.when(exists(-dx, -dy))(lambda k=k: halo_copy(*item, k).wait_recv())

    def end_halo(*item):
        for k in order:
            pl.when(exists(*DIRS[k]))(lambda k=k: halo_copy(*item, k).wait_send())

    def stencil(v, x, start, count):
        lane = lax.broadcasted_iota(jnp.int32, (count, LANES), 1)
        own = pl.ds(start, count)
        centre = [v[x, z, own, :] for z in range(parts)]
        fore = [pltpu.roll(c, 1, 1) for c in centre]
        back = [pltpu.roll(c, LANES - 1, 1) for c in centre]
        out = []
        for z in range(parts):
            near = jnp.where(lane == 0, fore[z - 1] if z > 0 else 0.0, fore[z])
            far = jnp.where(lane == LANES - 1, back[z + 1] if z + 1 < parts else 0.0, back[z])
            beside = v[x - 1, z, own, :] + v[x + 1, z, own, :]
            beside = beside + v[x, z, pl.ds(start - 1, count), :] + v[x, z, pl.ds(start + 1, count), :]
            beside = beside + (near + far)
            out.append((dmp[x, z, own, :] + (7.0 - MID)) * centre[z] - beside)
        return out, centre

    low = jnp.where(y_in[0], 0, PY)
    high = jnp.where(y_in[1], 2 * PY + rows, PY + rows)

    def fold(block):
        return jnp.sum(block.reshape(-1, 8, LANES), axis=0)

    def reach(h):
        return PY - h, -(-(rows + 2 * h) // 8) * 8

    def inside(x, start, count):
        row = lax.broadcasted_iota(jnp.int32, (count, LANES), 0) + start
        ok = jnp.logical_and(row >= low, row < high)
        if PX <= x < PX + half:
            return ok
        return jnp.logical_and(ok, x_in[0] if x < PX else x_in[1])

    def powers(head, work, with_dots=False):
        zero = jnp.zeros((8, LANES), jnp.float32)
        totals = []
        for k in range(1, ITERS + 1):
            h = ITERS - k
            start, count = reach(h)
            prev = head if k == 1 else work[k - 2]
            older = None if k == 1 else head if k == 2 else work[k - 3]
            row = lax.broadcasted_iota(jnp.int32, (count, LANES), 0) + start
            keep = jnp.logical_and(row >= PY, row < PY + rows)
            a, b = zero, zero
            for x in range(PX - h, PX + half + h):
                t, centre = stencil(prev, x, start, count)
                ok = inside(x, start, count)
                for z in range(parts):
                    if k == 1:
                        new = t[z] * (1.0 / HALF)
                    else:
                        new = t[z] * (2.0 / HALF) - older[x, z, pl.ds(start, count), :]
                    if h > 0:
                        new = jnp.where(ok, new, 0.0)
                    work[k - 1][x, z, pl.ds(start, count), :] = new
                    if with_dots and PX <= x < PX + half:
                        square, cross = centre[z] * centre[z], centre[z] * new
                        if h > 0:
                            square, cross = jnp.where(keep, square, 0.0), jnp.where(keep, cross, 0.0)
                        a = a + fold(square)
                        b = b + fold(cross)
            totals += [a, b]
        return totals

    inner = INNER if ny % INNER == 0 else 1
    extent = {"level": levels, "gx": nx, "outer": ny // inner, "inner": inner}
    here = {"level": level, "gx": gx, "outer": lax.div(yz, inner), "inner": lax.rem(yz, inner)}
    ring = {a: [here[a]] + [lax.rem(here[a] + off, n) for off in range(1, n)] for a, n in extent.items()}
    flows = []
    for axes in (("level",), ("gx", "outer", "inner")):
        peers, me, n = [{}], 0, 1
        for a in axes:
            peers = [dict(p, **{a: off}) for p in peers for off in range(extent[a])]
            me, n = me * extent[a] + here[a], n * extent[a]
        peers = [p for p in peers if any(p.values())]
        peers.sort(key=lambda p: -sum(min(off, extent[a] - off) for a, off in p.items()))
        flows.append((peers, me, n))

    def cast(s, turn):
        peers, me, n = flows[s]
        copies = []
        for p in peers:
            at = {a: ring[a][p.get(a, 0)] for a in extent}
            cell = slots[s].at[turn, pl.ds(me, 1), :]
            copies.append(pltpu.make_async_remote_copy(
                src_ref=cell, dst_ref=cell, send_sem=red_send[s].at[turn], recv_sem=red_recv[s].at[turn],
                device_id={"level": at["level"], "gx": at["gx"], "yz": at["outer"] * inner + at["inner"]}, device_id_type=MESH))
        return copies

    def gathered(s, turn):
        bulk = slots[s].at[turn, pl.ds(0, flows[s][2] - 1), :]
        return pltpu.make_async_remote_copy(
            src_ref=bulk, dst_ref=bulk, send_sem=red_send[s].at[turn], recv_sem=red_recv[s].at[turn],
            device_id={"level": 1 - level, "gx": gx, "yz": yz}, device_id_type=MESH)

    def reduce_all(accs, turn, outgoing, meanwhile):
        n = len(accs)
        size = -(-n // 8) * 8
        eye = lax.broadcasted_iota(jnp.int32, (size, LANES), 0) == lax.broadcasted_iota(jnp.int32, (size, LANES), 1)
        tall = jnp.concatenate([jnp.sum(a, axis=0, keepdims=True) for a in accs]
                               + [jnp.zeros((size - n, LANES), jnp.float32)] * (size > n), axis=0)
        col = jnp.sum(tall, axis=1, keepdims=True)
        line = jnp.sum(jnp.where(eye, col, 0.0), axis=0, keepdims=True)
        for s in range(len(flows)):
            slots[s][turn, pl.ds(flows[s][1], 1), :] = line
            for copy in cast(s, turn):
                copy.start()
            if s == 0 and turn == 0:
                meet(ROUNDS)
            if s == len(flows) - 1:
                for item in outgoing:
                    send_halo(*item)
                meanwhile()
            gathered(s, turn).wait_recv()
            line = jnp.sum(slots[s][turn], axis=0, keepdims=True)
        col = jnp.sum(jnp.where(eye, line, 0.0), axis=1, keepdims=True)
        wide = jnp.broadcast_to(col, (size, LANES))
        return [jnp.broadcast_to(wide[k:k + 1, :], (8, LANES)) for k in range(n)]

    def place(ref, f, part, z):
        return ref.at[0, pl.ds(part * half, half), :, slice(z * LANES, (z + 1) * LANES)]

    def across(f, z):
        return pltpu.make_async_remote_copy(
            src_ref=result.at[f, :, z], dst_ref=place(out_ref, f, level, z), send_sem=p_send.at[z], recv_sem=p_recv.at[z],
            device_id={"level": f, "gx": gx, "yz": yz}, device_id_type=MESH)

    def deliver(f):
        @pl.when(level != f)
        def _():
            for z in range(parts):
                across(f, z).start()

        @pl.when(level == f)
        def _():
            for z in range(parts):
                place(out_ref, f, level, z)[...] = result[f, :, z]

    pl.semaphore_wait(barrier, greeted)
    meet(0)
    starts = ((p0, PX, 0), (dmp, PX - 1, 1), (src, PX - 1, 2))
    for item, at in zip(starts, (0, 2, 1)):
        for copy in loads[at * parts:(at + 1) * parts]:
            copy.wait()
        send_halo(*item)
    for turn in range(1, ROUNDS):
        meet(turn)
    for item in starts:
        wait_halo(*item)

    start, count = reach(ITERS)
    for x in range(PX - ITERS, PX + half + ITERS):
        t, centre = stencil(p0, x, start, count)
        ok = inside(x, start, count)
        for z in range(parts):
            r = src[x, z, pl.ds(start, count), :] - (t[z] + (MID - 1.0) * centre[z])
            first[0, x, z, pl.ds(start, count), :] = jnp.where(ok, r, 0.0)
    accs = powers(first.at[0], (first.at[1], first.at[2], heads_p.at[0]), True)

    pending = list(starts)
    slot = len(starts)
    for turn in range(STEPS + 1):
        with_p, with_c = turn < STEPS, turn > 0
        outgoing, jobs = [], []
        if with_p:
            outgoing.append((heads_p.at[turn], ITERS, slot))
            jobs.append((heads_p.at[turn], work_p))
            slot += 1
        if with_p and with_c:
            outgoing.append((heads_c.at[turn - 1], ITERS, slot))
            jobs.append((heads_c.at[turn - 1], work_c))
            slot += 1

        def meanwhile(outgoing=outgoing, jobs=jobs):
            for item, (head, work) in zip(outgoing, jobs):
                wait_halo(*item)
                powers(head, [work.at[k] for k in range(ITERS)])

        pending += outgoing
        dots = reduce_all(accs, turn, outgoing, meanwhile)
        sets = [cg_coefficients(dots[6 * i:6 * i + 6]) for i in range(len(dots) // 6)]
        if with_p:
            rise_p, table_p = sets[0][0], shifted(sets[0][1])
        if with_c:
            rise_c, table_c = sets[-1][0], shifted(sets[-1][1])
        n_acc = 6 * ((turn + 1 < STEPS) + (turn < STEPS))

        def update(i, accs):
            x = i + PX
            accs = list(accs)
            for z in range(parts):
                for y in range(0, rows, 8):
                    near, wide = pl.ds(y, 8), pl.ds(PY + y, 8)
                    if with_p:
                        if turn == 0:
                            v = [first[j, x, z, wide, :] for j in range(ITERS)]
                        else:
                            v = [own_p[j, i, z, near, :] for j in range(ITERS)]
                        v.append(heads_p[turn, x, z, wide, :])
                        v += [work_p[k, x, z, wide, :] for k in range(ITERS)]
                        before = p0[x, z, wide, :] if turn == 0 else sums[0, i, z, near, :]
                        after = before + combine(rise_p, v)
                        if turn + 1 < STEPS:
                            sums[0, i, z, near, :] = after
                        else:
                            result[0, i, z, near, :] = after
                        change = [combine(row, v) for row in table_p]
                    if with_c:
                        u = [own_c[j, i, z, near, :] for j in range(ITERS)]
                        before = p0[x, z, wide, :] if turn == 1 else sums[1, i, z, near, :]
                        after = before + combine(rise_c, u)
                        if turn < STEPS:
                            sums[1, i, z, near, :] = after
                            u.append(heads_c[turn - 1, x, z, wide, :])
                            u += [work_c[k, x, z, wide, :] for k in range(ITERS)]
                        else:
                            result[1, i, z, near, :] = after
                    if turn == STEPS:
                        continue
                    news = []
                    if turn + 1 < STEPS:
                        fresh = [a - b for a, b in zip(v, change)]
                        for j in range(ITERS):
                            own_p[j, i, z, near, :] = fresh[j]
                        heads_p[turn + 1, x, z, wide, :] = fresh[ITERS]
                        news.append(fresh)
                    if turn == 0:
                        ground = v[:ITERS + 1]
                    else:
                        if turn == 1:
                            ground = [first[j, x, z, wide, :] for j in range(ITERS)] + [heads_p[0, x, z, wide, :]]
                        else:
                            ground = [base[j, i, z, near, :] for j in range(ITERS + 1)]
                        ground = [a - combine(row, u) for a, row in zip(ground, table_c)]
                        if turn + 1 < STEPS:
                            for j in range(ITERS + 1):
                                base[j, i, z, near, :] = ground[j]
                    fresh = [a + 0.5 * b for a, b in zip(ground, change)]
                    for j in range(ITERS):
                        own_c[j, i, z, near, :] = fresh[j]
                    heads_c[turn, x, z, wide, :] = fresh[ITERS]
                    news.append(fresh)
                    for f, fresh in enumerate(news):
                        for j in range(ITERS):
                            accs[6 * f + 2 * j] = accs[6 * f + 2 * j] + fresh[j] * fresh[j]
                            accs[6 * f + 2 * j + 1] = accs[6 * f + 2 * j + 1] + fresh[j] * fresh[j + 1]
            return tuple(accs)

        accs = lax.fori_loop(0, half, update, (jnp.zeros((8, LANES), jnp.float32),) * n_acc)
        if turn == STEPS - 1:
            deliver(0)
    deliver(1)
    for item in pending:
        end_halo(*item)
    for turn in range(STEPS + 1):
        for s in range(len(flows)):
            gathered(s, turn).wait_send()
    for f in range(2):
        for z in range(parts):
            pl.when(level != f)(lambda f=f, z=z: across(f, z).wait_send())
            pl.when(level == f)(lambda f=f, z=z: across(f, z).wait_recv())


def solution(mesh):
    levels, nx, ny = mesh.shape["level"], mesh.shape["gx"], mesh.shape["yz"]

    def per_device(init_field, source, damping):
        deep, rows, wide = init_field.shape
        half, parts = deep // levels, wide // LANES
        padded = (half + 2 * PX, parts, rows + 2 * PY, LANES)
        plain = (half, parts, rows, LANES)
        counts = (levels, nx * ny)
        turns = STEPS + 1
        dma = pltpu.SemaphoreType.DMA
        exchanges = 3 + 2 * STEPS - 1
        vmem = lambda n, shape: pltpu.VMEM((n,) + shape, jnp.float32)
        return pl.pallas_call(
            functools.partial(body, (levels, nx, ny)),
            out_shape=pltpu.VMEM((1, deep, rows, wide), jnp.float32),
            in_specs=[pl.BlockSpec(memory_space=pltpu.HBM)] * 3,
            out_specs=pl.BlockSpec(memory_space=pltpu.VMEM),
            scratch_shapes=[
                pltpu.VMEM(padded, jnp.float32),
                pltpu.VMEM(padded, jnp.float32),
                pltpu.VMEM(padded, jnp.float32),
                vmem(ITERS, padded),
                vmem(STEPS, padded),
                vmem(STEPS, padded),
                vmem(ITERS, plain),
                vmem(ITERS, plain),
                vmem(ITERS + 1, plain),
                vmem(ITERS, padded),
                vmem(ITERS, padded),
                vmem(2, plain),
                vmem(2, plain),
                [pltpu.VMEM((turns, n, LANES), jnp.float32) for n in counts],
                dma((3, parts)),
                dma((exchanges, 8)),
                dma((exchanges, 8)),
                [dma((turns,)) for n in counts],
                [dma((turns,)) for n in counts],
                dma((parts,)),
                dma((parts,)),
                pltpu.SemaphoreType.REGULAR((ROUNDS,)),
            ],
            compiler_params=pltpu.CompilerParams(has_side_effects=True, collective_id=0),
        )(init_field, source, damping)

    spec = P("gx", "yz", None)
    return jax.shard_map(
        per_device, mesh=mesh, in_specs=(spec, spec, spec),
        out_specs=P("level", "gx", "yz", None), check_vma=False,
    )
```

```python
import functools

import jax
import jax.numpy as jnp
from jax import lax
from jax.experimental import pallas as pl
from jax.experimental.pallas import tpu as pltpu
from jax.sharding import PartitionSpec as P

STEPS = 3
ITERS = 3
ROUNDS = 5
INNER = 4
PX = 4
PY = 8
LANES = 128
MID = 8.025
HALF = 6.975
MESH = pl.DeviceIdType.MESH
DIRS = ((-1, 0), (1, 0), (0, -1), (0, 1), (-1, -1), (-1, 1), (1, -1), (1, 1))


def times_a(c):
    out = [MID * v for v in c] + [jnp.zeros_like(c[0])]
    for k, v in enumerate(c):
        if k == 0:
            out[1] = out[1] + HALF * v
        else:
            out[k + 1] = out[k + 1] + (0.5 * HALF) * v
            out[k - 1] = out[k - 1] + (0.5 * HALF) * v
    return out


def plus(a, b):
    short, long = (a, b) if len(a) < len(b) else (b, a)
    return [x + y for x, y in zip(short, long)] + long[len(short):]


def scaled(s, a):
    return [s * x for x in a]


def cg_coefficients(dots):
    m = [dots[0], dots[1], 2.0 * dots[2] - dots[0], 2.0 * dots[3] - dots[1],
         2.0 * dots[4] - dots[0], 2.0 * dots[5] - dots[1]]

    def inner(a, b):
        total = None
        for i, x in enumerate(a):
            for j, y in enumerate(b):
                term = (x * y) * (0.5 * (m[i + j] + m[abs(i - j)]))
                total = term if total is None else total + term
        return total

    one = jnp.ones_like(m[0])
    resid = [one]
    direction = resid
    image = times_a(resid)
    along = image
    norm_now = m[0]
    alpha = norm_now / inner(resid, image)
    answer = None
    for step in range(ITERS):
        move = scaled(alpha, direction)
        answer = move if answer is None else plus(answer, move)
        if step + 1 < ITERS:
            resid = plus(resid, scaled(-alpha, along))
            image = times_a(resid)
            norm_next = inner(resid, resid)
            product = inner(resid, image)
            ratio = norm_next / norm_now
            alpha = norm_next / (product - ratio * norm_next / alpha)
            direction = plus(resid, scaled(ratio, direction))
            along = plus(image, scaled(ratio, along))
            norm_now = norm_next
    change = plus(times_a(answer), scaled(-1.0, answer))
    return answer, change


def shifted(c, v):
    t, w = v[:ITERS + 1], v[ITERS + 1:]
    one, two = 0.5 * c[1], 0.5 * c[2]
    even, odd, gap = t[0] + t[2], t[1] + t[3], t[0] - t[2]
    return [
        c[0] * t[0] + c[1] * t[1] + (c[2] * t[2] + c[3] * t[3]),
        c[0] * t[1] + one * even + (two * odd + c[3] * w[0]),
        c[0] * t[2] + one * odd + (two * gap + c[2] * w[0]) + c[3] * w[1],
        c[0] * t[3] + c[1] * w[0] + (c[2] * w[1] + c[3] * w[2]),
    ]


def combine(c, v):
    total = None
    for a, b in zip(c, v):
        total = a * b if total is None else total + a * b
    return total


def body(sizes, init_ref, source_ref, damp_ref, out_ref, p0, src, dmp, first, heads_p, heads_c, own_p, own_c,
         base, work_p, work_c, sums, result, far_c, slots, in_sem, send_sem, recv_sem, red_send, red_recv, p_send, p_recv, up_send, up_recv,
         met):
    levels, nx, ny = sizes
    half = own_p.shape[1]
    parts = p0.shape[1]
    rows = own_p.shape[3]
    level, gx, yz = lax.axis_index("level"), lax.axis_index("gx"), lax.axis_index("yz")
    xpos = gx * levels + level
    xcount = nx * levels
    x_in = (xpos > 0, xpos < xcount - 1)
    y_in = (yz > 0, yz < ny - 1)

    def exists(dx, dy):
        ok = None
        for d, at, count in ((dx, xpos, xcount), (dy, yz, ny)):
            if d != 0:
                c = at + d >= 0 if d < 0 else at + d < count
                ok = c if ok is None else jnp.logical_and(ok, c)
        return ok

    def beside(dx, dy):
        to = xpos + dx
        return {"level": lax.rem(to + xcount, levels), "gx": lax.div(to + xcount, levels) - nx, "yz": yz + dy}

    mine = pl.ds(level * half, half)
    loads = []
    for i, (ref, buf) in enumerate(((init_ref, p0), (source_ref, src), (damp_ref, dmp))):
        for z in range(parts):
            copy = pltpu.make_async_copy(ref.at[mine, :, slice(z * LANES, (z + 1) * LANES)],
                                         buf.at[PX:PX + half, z, PY:PY + rows, :], in_sem.at[i, z])
            copy.start()
            loads.append(copy)

    def signal_all(sem, steps):
        count = 0
        for dx, dy in steps:
            ok = exists(dx, dy)
            count = count + jnp.where(ok, 1, 0)

            @pl.when(ok)
            def _(dx=dx, dy=dy):
                pl.semaphore_signal(sem, inc=1, device_id=beside(dx, dy), device_id_type=MESH)
        return count

    def meet(turn):
        if turn > 0:
            far = 2 ** (turn - 1)
            count = 0
            for d in (-far, far):
                count = count + jnp.where(exists(0, d), 1, 0)
            pl.semaphore_wait(met.at[turn - 1], count)
        if turn < ROUNDS:
            signal_all(met.at[turn], [(0, -2 ** turn), (0, 2 ** turn)])

    barrier = pltpu.get_barrier_semaphore()
    greeted = signal_all(barrier, DIRS + tuple((d, 0) for d in range(1 - xcount, xcount) if abs(d) > 1))

    zero_x = jnp.zeros((PX,) + tuple(p0.shape[1:]), jnp.float32)
    zero_y = jnp.zeros((p0.shape[0], parts, PY, LANES), jnp.float32)
    for buf in [p0] + [heads_p.at[n] for n in range(STEPS)] + [heads_c.at[n] for n in range(STEPS - 1)]:
        @pl.when(jnp.logical_not(x_in[0]))
        def _(buf=buf):
            buf[0:PX] = zero_x

        @pl.when(jnp.logical_not(x_in[1]))
        def _(buf=buf):
            buf[PX + half:] = zero_x

        @pl.when(jnp.logical_not(y_in[0]))
        def _(buf=buf):
            buf[:, :, 0:PY, :] = zero_y

        @pl.when(jnp.logical_not(y_in[1]))
        def _(buf=buf):
            buf[:, :, PY + rows:, :] = zero_y

    def halo_copy(buf, width, slot, k):
        dx, dy = DIRS[k]
        w = width if 0 in (dx, dy) else width - 1

        def spans(d, pad, size):
            if d == 0:
                return slice(pad, pad + size), slice(pad, pad + size)
            if d < 0:
                return slice(pad, pad + w), slice(pad + size, pad + size + w)
            return slice(pad + size - w, pad + size), slice(pad - w, pad)

        sx, tx = spans(dx, PX, half)
        sy, ty = spans(dy, PY, rows)
        return pltpu.make_async_remote_copy(
            src_ref=buf.at[sx, :, sy, :], dst_ref=buf.at[tx, :, ty, :],
            send_sem=send_sem.at[slot, k], recv_sem=recv_sem.at[slot, k],
            device_id=beside(dx, dy), device_id_type=MESH,
        )

    order = (2, 3, 4, 5, 6, 7, 0, 1)

    def send_halo(*item):
        for k in order:
            pl.when(exists(*DIRS[k]))(lambda k=k: halo_copy(*item, k).start())

    def wait_halo(*item):
        for k in order:
            dx, dy = DIRS[k]
            pl.when(exists(-dx, -dy))(lambda k=k: halo_copy(*item, k).wait_recv())

    def end_halo(*item):
        for k in order:
            pl.when(exists(*DIRS[k]))(lambda k=k: halo_copy(*item, k).wait_send())

    def around(v, x, start, count):
        lane = lax.broadcasted_iota(jnp.int32, (count, LANES), 1)
        own = pl.ds(start, count)
        centre = [v[x, z, own, :] for z in range(parts)]
        fore = [pltpu.roll(c, 1, 1) for c in centre]
        back = [pltpu.roll(c, LANES - 1, 1) for c in centre]
        out = []
        for z in range(parts):
            near = jnp.where(lane == 0, fore[z - 1] if z > 0 else 0.0, fore[z])
            far = jnp.where(lane == LANES - 1, back[z + 1] if z + 1 < parts else 0.0, back[z])
            beside = v[x - 1, z, own, :] + v[x + 1, z, own, :]
            beside = beside + v[x, z, pl.ds(start - 1, count), :] + v[x, z, pl.ds(start + 1, count), :]
            beside = beside + (near + far)
            out.append(beside)
        return out, centre

    def stencil(v, x, start, count):
        out, centre = around(v, x, start, count)
        own = pl.ds(start, count)
        return [(dmp[x, z, own, :] + (7.0 - MID)) * centre[z] - out[z] for z in range(parts)], centre

    low = jnp.where(y_in[0], 0, PY)
    high = jnp.where(y_in[1], 2 * PY + rows, PY + rows)

    def fold(block):
        return jnp.sum(block.reshape(-1, 8, LANES), axis=0)

    def reach(h):
        return PY - h, -(-(rows + 2 * h) // 8) * 8

    def inside(x, start, count):
        row = lax.broadcasted_iota(jnp.int32, (count, LANES), 0) + start
        ok = jnp.logical_and(row >= low, row < high)
        if PX <= x < PX + half:
            return ok
        return jnp.logical_and(ok, x_in[0] if x < PX else x_in[1])

    def powers(head, work, with_dots=False):
        zero = jnp.zeros((8, LANES), jnp.float32)
        totals = []
        for k in range(1, ITERS + 1):
            h = ITERS - k
            start, count = reach(h)
            prev = head if k == 1 else work[k - 2]
            older = None if k == 1 else head if k == 2 else work[k - 3]
            row = lax.broadcasted_iota(jnp.int32, (count, LANES), 0) + start
            keep = jnp.logical_and(row >= PY, row < PY + rows)
            a, b = zero, zero
            for x in range(PX - h, PX + half + h):
                t, centre = stencil(prev, x, start, count)
                ok = inside(x, start, count)
                for z in range(parts):
                    if k == 1:
                        new = t[z] * (1.0 / HALF)
                    else:
                        new = t[z] * (2.0 / HALF) - older[x, z, pl.ds(start, count), :]
                    if h > 0:
                        new = jnp.where(ok, new, 0.0)
                    work[k - 1][x, z, pl.ds(start, count), :] = new
                    if with_dots and PX <= x < PX + half:
                        square, cross = centre[z] * centre[z], centre[z] * new
                        if h > 0:
                            square, cross = jnp.where(keep, square, 0.0), jnp.where(keep, cross, 0.0)
                        a = a + fold(square)
                        b = b + fold(cross)
            totals += [a, b]
        return totals

    inner = INNER if ny % INNER == 0 else 1
    extent = {"level": levels, "gx": nx, "outer": ny // inner, "inner": inner}
    here = {"level": level, "gx": gx, "outer": lax.div(yz, inner), "inner": lax.rem(yz, inner)}
    ring = {a: [here[a]] + [lax.rem(here[a] + off, n) for off in range(1, n)] for a, n in extent.items()}
    flows = []
    for axes in (("level",), ("gx", "outer", "inner")):
        peers, me, n = [{}], 0, 1
        for a in axes:
            peers = [dict(p, **{a: off}) for p in peers for off in range(extent[a])]
            me, n = me * extent[a] + here[a], n * extent[a]
        peers = [p for p in peers if any(p.values())]
        peers.sort(key=lambda p: -sum(min(off, extent[a] - off) for a, off in p.items()))
        flows.append((peers, me, n))

    def cast(s, turn):
        peers, me, n = flows[s]
        copies = []
        for p in peers:
            at = {a: ring[a][p.get(a, 0)] for a in extent}
            cell = slots[s].at[turn, pl.ds(me, 1), :]
            copies.append(pltpu.make_async_remote_copy(
                src_ref=cell, dst_ref=cell, send_sem=red_send[s].at[turn], recv_sem=red_recv[s].at[turn],
                device_id={"level": at["level"], "gx": at["gx"], "yz": at["outer"] * inner + at["inner"]}, device_id_type=MESH))
        return copies

    def gathered(s, turn):
        bulk = slots[s].at[turn, pl.ds(0, flows[s][2] - 1), :]
        return pltpu.make_async_remote_copy(
            src_ref=bulk, dst_ref=bulk, send_sem=red_send[s].at[turn], recv_sem=red_recv[s].at[turn],
            device_id={"level": 1 - level, "gx": gx, "yz": yz}, device_id_type=MESH)

    def reduce_all(accs, turn, meanwhile):
        n = len(accs)
        size = -(-n // 8) * 8
        eye = lax.broadcasted_iota(jnp.int32, (size, LANES), 0) == lax.broadcasted_iota(jnp.int32, (size, LANES), 1)
        tall = jnp.concatenate([jnp.sum(a, axis=0, keepdims=True) for a in accs]
                               + [jnp.zeros((size - n, LANES), jnp.float32)] * (size > n), axis=0)
        col = jnp.sum(tall, axis=1, keepdims=True)
        line = jnp.sum(jnp.where(eye, col, 0.0), axis=0, keepdims=True)
        for s in range(len(flows)):
            slots[s][turn, pl.ds(flows[s][1], 1), :] = line

            def start(s=s):
                for copy in cast(s, turn):
                    copy.start()

            def finish(s=s):
                gathered(s, turn).wait_recv()

            last = s == len(flows) - 1
            alone = last and turn == STEPS
            pl.when(level == 1)(start) if alone else start()
            if s == 0 and turn == 0:
                meet(ROUNDS)
            if last:
                meanwhile()
            pl.when(level == 1)(finish) if alone else finish()
            line = jnp.sum(slots[s][turn], axis=0, keepdims=True)
        col = jnp.sum(jnp.where(eye, line, 0.0), axis=1, keepdims=True)
        wide = jnp.broadcast_to(col, (size, LANES))
        return [jnp.broadcast_to(wide[k:k + 1, :], (8, LANES)) for k in range(n)]

    def place(part, z):
        return out_ref.at[0, pl.ds(part * half, half), :, slice(z * LANES, (z + 1) * LANES)]

    def across(z):
        return pltpu.make_async_remote_copy(
            src_ref=result.at[:, z], dst_ref=place(1, z), send_sem=p_send.at[z], recv_sem=p_recv.at[z],
            device_id={"level": 0, "gx": gx, "yz": yz}, device_id_type=MESH)

    def upward(k):
        source, target = ((own_c, far_c.at[0:ITERS]), (sums.at[1], far_c.at[ITERS]))[k]
        return pltpu.make_async_remote_copy(
            src_ref=source, dst_ref=target, send_sem=up_send.at[k], recv_sem=up_recv.at[k],
            device_id={"level": 1, "gx": gx, "yz": yz}, device_id_type=MESH)

    def trade():
        @pl.when(level == 0)
        def _():
            for k in range(2):
                upward(k).start()
            for z in range(parts):
                place(0, z)[...] = result[:, z]

        @pl.when(level == 1)
        def _():
            for z in range(parts):
                across(z).start()

    for copy in loads:
        copy.wait()
    for x in range(PX, PX + half):
        for z in range(parts):
            src[x, z, PY:PY + rows, :] = src[x, z, PY:PY + rows, :] - dmp[x, z, PY:PY + rows, :] * p0[x, z, PY:PY + rows, :]
    pl.semaphore_wait(barrier, greeted)
    meet(0)
    starts = ((p0, PX, 0), (src, ITERS, 1), (dmp, ITERS - 1, 2))
    for item in starts:
        send_halo(*item)
    for turn in range(1, ROUNDS):
        meet(turn)
    for item in starts:
        wait_halo(*item)

    start, count = reach(ITERS)
    for x in range(PX - ITERS, PX + half + ITERS):
        t, centre = around(p0, x, start, count)
        ok = inside(x, start, count)
        for z in range(parts):
            r = src[x, z, pl.ds(start, count), :] - (6.0 * centre[z] - t[z])
            first[0, x, z, pl.ds(start, count), :] = jnp.where(ok, r, 0.0)
    accs = powers(first.at[0], (first.at[1], first.at[2], heads_p.at[0]), True)

    pending = list(starts)
    slot = len(starts)
    for turn in range(STEPS + 1):
        with_p, with_c = turn < STEPS, turn > 0
        jobs = []
        for on, head, work in ((with_p, heads_p.at[turn], work_p), (with_p and with_c, heads_c.at[turn - 1], work_c)):
            if on:
                jobs.append(((head, ITERS, slot), work))
                slot += 1
        if jobs:
            send_halo(*jobs[0][0])

        def meanwhile(turn=turn, jobs=jobs):
            for item, _ in jobs[1:]:
                send_halo(*item)
            if turn == STEPS:
                trade()
            for item, work in jobs:
                wait_halo(*item)
                powers(item[0], [work.at[k] for k in range(ITERS)])

        pending += [item for item, _ in jobs]
        dots = reduce_all(accs, turn, meanwhile)
        sets = [cg_coefficients(dots[6 * i:6 * i + 6]) for i in range(len(dots) // 6)]
        if with_p:
            rise_p, step_p = sets[0]
        if with_c:
            rise_c, step_c = sets[-1]
        n_acc = 6 * ((turn + 1 < STEPS) + (turn < STEPS))

        def update(i, accs):
            x = i + PX
            accs = list(accs)
            for z in range(parts):
                for y in range(0, rows, 8):
                    near, wide = pl.ds(y, 8), pl.ds(PY + y, 8)
                    if with_p:
                        if turn == 0:
                            v = [first[j, x, z, wide, :] for j in range(ITERS)]
                        else:
                            v = [own_p[j, i, z, near, :] for j in range(ITERS)]
                        v.append(heads_p[turn, x, z, wide, :])
                        v += [work_p[k, x, z, wide, :] for k in range(ITERS)]
                        before = p0[x, z, wide, :] if turn == 0 else sums[0, i, z, near, :]
                        after = before + combine(rise_p, v)
                        if turn + 1 < STEPS:
                            sums[0, i, z, near, :] = after
                        else:
                            result[i, z, near, :] = after
                        change = shifted(step_p, v)
                    if with_c:
                        u = [own_c[j, i, z, near, :] for j in range(ITERS)]
                        before = p0[x, z, wide, :] if turn == 1 else sums[1, i, z, near, :]
                        sums[1, i, z, near, :] = before + combine(rise_c, u)
                        u.append(heads_c[turn - 1, x, z, wide, :])
                        u += [work_c[k, x, z, wide, :] for k in range(ITERS)]
                    news = []
                    if turn + 1 < STEPS:
                        fresh = [a - b for a, b in zip(v, change)]
                        for j in range(ITERS):
                            own_p[j, i, z, near, :] = fresh[j]
                        heads_p[turn + 1, x, z, wide, :] = fresh[ITERS]
                        news.append(fresh)
                    if turn == 0:
                        ground = v[:ITERS + 1]
                    else:
                        if turn == 1:
                            ground = [first[j, x, z, wide, :] for j in range(ITERS)] + [heads_p[0, x, z, wide, :]]
                        else:
                            ground = [base[j, i, z, near, :] for j in range(ITERS + 1)]
                        ground = [a - b for a, b in zip(ground, shifted(step_c, u))]
                        if turn + 1 < STEPS:
                            for j in range(ITERS + 1):
                                base[j, i, z, near, :] = ground[j]
                    fresh = [a + 0.5 * b for a, b in zip(ground, change)]
                    for j in range(ITERS):
                        own_c[j, i, z, near, :] = fresh[j]
                    heads_c[turn, x, z, wide, :] = fresh[ITERS]
                    news.append(fresh)
                    for f, fresh in enumerate(news):
                        for j in range(ITERS):
                            accs[6 * f + 2 * j] = accs[6 * f + 2 * j] + fresh[j] * fresh[j]
                            accs[6 * f + 2 * j + 1] = accs[6 * f + 2 * j + 1] + fresh[j] * fresh[j + 1]
            return tuple(accs)

        def last(i, carry):
            for z in range(parts):
                for y in range(0, rows, 8):
                    near, lanes = pl.ds(y, 8), slice(z * LANES, (z + 1) * LANES)
                    out_ref[0, half + i, near, lanes] = sums[1, i, z, near, :] + combine(
                        rise_c, [own_c[j, i, z, near, :] for j in range(ITERS)])
                    out_ref[0, i, near, lanes] = far_c[ITERS, i, z, near, :] + combine(
                        rise_c, [far_c[j, i, z, near, :] for j in range(ITERS)])
            return carry

        if turn < STEPS:
            accs = lax.fori_loop(0, half, update, (jnp.zeros((8, LANES), jnp.float32),) * n_acc)
        else:
            @pl.when(level == 1)
            def _():
                for k in range(2):
                    upward(k).wait_recv()
                lax.fori_loop(0, half, last, 0)
    for item in pending:
        end_halo(*item)
    for turn in range(STEPS + 1):
        gathered(0, turn).wait_send()
        if turn < STEPS:
            gathered(1, turn).wait_send()
        else:
            pl.when(level == 1)(lambda turn=turn: gathered(1, turn).wait_send())
    for z in range(parts):
        pl.when(level == 1)(lambda z=z: across(z).wait_send())
        pl.when(level == 0)(lambda z=z: across(z).wait_recv())
    for k in range(2):
        pl.when(level == 0)(lambda k=k: upward(k).wait_send())


def solution(mesh):
    levels, nx, ny = mesh.shape["level"], mesh.shape["gx"], mesh.shape["yz"]

    def per_device(init_field, source, damping):
        deep, rows, wide = init_field.shape
        half, parts = deep // levels, wide // LANES
        padded = (half + 2 * PX, parts, rows + 2 * PY, LANES)
        plain = (half, parts, rows, LANES)
        counts = (levels, nx * ny)
        turns = STEPS + 1
        dma = pltpu.SemaphoreType.DMA
        exchanges = 3 + 2 * STEPS - 1
        vmem = lambda n, shape: pltpu.VMEM((n,) + shape, jnp.float32)
        return pl.pallas_call(
            functools.partial(body, (levels, nx, ny)),
            out_shape=pltpu.VMEM((1, deep, rows, wide), jnp.float32),
            in_specs=[pl.BlockSpec(memory_space=pltpu.HBM)] * 3,
            out_specs=pl.BlockSpec(memory_space=pltpu.VMEM),
            scratch_shapes=[
                pltpu.VMEM(padded, jnp.float32),
                pltpu.VMEM(padded, jnp.float32),
                pltpu.VMEM(padded, jnp.float32),
                vmem(ITERS, padded),
                vmem(STEPS, padded),
                vmem(STEPS, padded),
                vmem(ITERS, plain),
                vmem(ITERS, plain),
                vmem(ITERS + 1, plain),
                vmem(ITERS, padded),
                vmem(ITERS, padded),
                vmem(2, plain),
                pltpu.VMEM(plain, jnp.float32),
                vmem(ITERS + 1, plain),
                [pltpu.VMEM((turns, n, LANES), jnp.float32) for n in counts],
                dma((3, parts)),
                dma((exchanges, 8)),
                dma((exchanges, 8)),
                [dma((turns,)) for n in counts],
                [dma((turns,)) for n in counts],
                dma((parts,)),
                dma((parts,)),
                dma((2,)),
                dma((2,)),
                pltpu.SemaphoreType.REGULAR((ROUNDS,)),
            ],
            compiler_params=pltpu.CompilerParams(has_side_effects=True, collective_id=0),
        )(init_field, source, damping)

    spec = P("gx", "yz", None)
    return jax.shard_map(
        per_device, mesh=mesh, in_specs=(spec, spec, spec),
        out_specs=P("level", "gx", "yz", None), check_vma=False,
    )
```

```python
import functools

import jax
import jax.numpy as jnp
from jax import lax
from jax.experimental import pallas as pl
from jax.experimental.pallas import tpu as pltpu
from jax.sharding import PartitionSpec as P

STEPS = 3
ITERS = 3
ROUNDS = 3
INNER = 4
PX = 4
PY = 8
LANES = 128
MID = 8.025
HALF = 6.975
MESH = pl.DeviceIdType.MESH
DIRS = ((-1, 0), (1, 0), (0, -1), (0, 1), (-1, -1), (-1, 1), (1, -1), (1, 1))


def times_a(c):
    out = [MID * v for v in c] + [jnp.zeros_like(c[0])]
    for k, v in enumerate(c):
        if k == 0:
            out[1] = out[1] + HALF * v
        else:
            out[k + 1] = out[k + 1] + (0.5 * HALF) * v
            out[k - 1] = out[k - 1] + (0.5 * HALF) * v
    return out


def plus(a, b):
    short, long = (a, b) if len(a) < len(b) else (b, a)
    return [x + y for x, y in zip(short, long)] + long[len(short):]


def scaled(s, a):
    return [s * x for x in a]


def cg_coefficients(dots):
    m = [dots[0], dots[1], 2.0 * dots[2] - dots[0], 2.0 * dots[3] - dots[1],
         2.0 * dots[4] - dots[0], 2.0 * dots[5] - dots[1]]

    def inner(a, b):
        total = None
        for i, x in enumerate(a):
            for j, y in enumerate(b):
                term = (x * y) * (0.5 * (m[i + j] + m[abs(i - j)]))
                total = term if total is None else total + term
        return total

    one = jnp.ones_like(m[0])
    resid = [one]
    direction = resid
    image = times_a(resid)
    along = image
    norm_now = m[0]
    alpha = norm_now / inner(resid, image)
    answer = None
    for step in range(ITERS):
        move = scaled(alpha, direction)
        answer = move if answer is None else plus(answer, move)
        if step + 1 < ITERS:
            resid = plus(resid, scaled(-alpha, along))
            image = times_a(resid)
            norm_next = inner(resid, resid)
            product = inner(resid, image)
            ratio = norm_next / norm_now
            alpha = norm_next / (product - ratio * norm_next / alpha)
            direction = plus(resid, scaled(ratio, direction))
            along = plus(image, scaled(ratio, along))
            norm_now = norm_next
    change = plus(times_a(answer), scaled(-1.0, answer))
    return answer, change


def shifted(c, v):
    t, w = v[:ITERS + 1], v[ITERS + 1:]
    one, two = 0.5 * c[1], 0.5 * c[2]
    even, odd, gap = t[0] + t[2], t[1] + t[3], t[0] - t[2]
    return [
        c[0] * t[0] + c[1] * t[1] + (c[2] * t[2] + c[3] * t[3]),
        c[0] * t[1] + one * even + (two * odd + c[3] * w[0]),
        c[0] * t[2] + one * odd + (two * gap + c[2] * w[0]) + c[3] * w[1],
        c[0] * t[3] + c[1] * w[0] + (c[2] * w[1] + c[3] * w[2]),
    ]


def combine(c, v):
    total = None
    for a, b in zip(c, v):
        total = a * b if total is None else total + a * b
    return total


def body(sizes, init_ref, source_ref, damp_ref, out_ref, p0, src, dmp, first, heads_p, heads_c, own_p, own_c,
         base, work_p, work_c, sums, result, far_c, slots, in_sem, send_sem, recv_sem, red_send, red_recv, p_send, p_recv, up_send, up_recv,
         met):
    levels, nx, ny = sizes
    half = own_p.shape[1]
    parts = p0.shape[1]
    rows = own_p.shape[3]
    level, gx, yz = lax.axis_index("level"), lax.axis_index("gx"), lax.axis_index("yz")
    xpos = gx * levels + level
    xcount = nx * levels
    x_in = (xpos > 0, xpos < xcount - 1)
    y_in = (yz > 0, yz < ny - 1)

    def exists(dx, dy):
        ok = None
        for d, at, count in ((dx, xpos, xcount), (dy, yz, ny)):
            if d != 0:
                c = at + d >= 0 if d < 0 else at + d < count
                ok = c if ok is None else jnp.logical_and(ok, c)
        return ok

    def beside(dx, dy):
        to = xpos + dx
        return {"level": lax.rem(to + xcount, levels), "gx": lax.div(to + xcount, levels) - nx, "yz": yz + dy}

    mine = pl.ds(level * half, half)
    loads = []
    for i, (ref, buf) in enumerate(((init_ref, p0), (source_ref, src), (damp_ref, dmp))):
        for z in range(parts):
            copy = pltpu.make_async_copy(ref.at[mine, :, slice(z * LANES, (z + 1) * LANES)],
                                         buf.at[PX:PX + half, z, PY:PY + rows, :], in_sem.at[i, z])
            copy.start()
            loads.append(copy)

    def signal_all(sem, steps):
        count = 0
        for dx, dy in steps:
            ok = exists(dx, dy)
            count = count + jnp.where(ok, 1, 0)

            @pl.when(ok)
            def _(dx=dx, dy=dy):
                pl.semaphore_signal(sem, inc=1, device_id=beside(dx, dy), device_id_type=MESH)
        return count

    inner = INNER if ny % INNER == 0 else 1
    extent = {"level": levels, "gx": nx, "outer": ny // inner, "inner": inner}
    here = {"level": level, "gx": gx, "outer": lax.div(yz, inner), "inner": lax.rem(yz, inner)}
    ring = {a: [here[a]] + [lax.rem(here[a] + off, n) for off in range(1, n)] for a, n in extent.items()}
    deep = extent["outer"]
    rounds = ([(0, k) for k in range(1, inner)] + [(1, 0), (deep - 1, 0)],
              [(1, 0), (2, 0), (deep - 2, 0), (deep - 1, 0)],
              [(k, 0) for k in range(3, deep - 2)])

    def call(sem, steps):
        for far, near in steps:
            pl.semaphore_signal(sem, inc=1, device_id_type=MESH, device_id={
                "level": level, "gx": gx, "yz": ring["outer"][far] * inner + ring["inner"][near]})

    def meet(turn):
        if turn > 0:
            pl.semaphore_wait(met.at[turn - 1], len(rounds[turn - 1]))
        if turn < ROUNDS:
            call(met.at[turn], rounds[turn])

    barrier = pltpu.get_barrier_semaphore()
    greeted = signal_all(barrier, DIRS + tuple((d, 0) for d in range(1 - xcount, xcount) if abs(d) > 1)) + len(rounds[0])
    call(barrier, rounds[0])

    zero_x = jnp.zeros((PX,) + tuple(p0.shape[1:]), jnp.float32)
    zero_y = jnp.zeros((p0.shape[0], parts, PY, LANES), jnp.float32)
    for buf in [p0] + [heads_p.at[n] for n in range(STEPS)] + [heads_c.at[n] for n in range(STEPS - 1)]:
        @pl.when(jnp.logical_not(x_in[0]))
        def _(buf=buf):
            buf[0:PX] = zero_x

        @pl.when(jnp.logical_not(x_in[1]))
        def _(buf=buf):
            buf[PX + half:] = zero_x

        @pl.when(jnp.logical_not(y_in[0]))
        def _(buf=buf):
            buf[:, :, 0:PY, :] = zero_y

        @pl.when(jnp.logical_not(y_in[1]))
        def _(buf=buf):
            buf[:, :, PY + rows:, :] = zero_y

    def halo_copy(buf, width, slot, k):
        dx, dy = DIRS[k]
        w = width if 0 in (dx, dy) else width - 1

        def spans(d, pad, size):
            if d == 0:
                return slice(pad, pad + size), slice(pad, pad + size)
            if d < 0:
                return slice(pad, pad + w), slice(pad + size, pad + size + w)
            return slice(pad + size - w, pad + size), slice(pad - w, pad)

        sx, tx = spans(dx, PX, half)
        sy, ty = spans(dy, PY, rows)
        return pltpu.make_async_remote_copy(
            src_ref=buf.at[sx, :, sy, :], dst_ref=buf.at[tx, :, ty, :],
            send_sem=send_sem.at[slot, k], recv_sem=recv_sem.at[slot, k],
            device_id=beside(dx, dy), device_id_type=MESH,
        )

    order = (2, 3, 4, 5, 6, 7, 0, 1)

    def send_halo(*item):
        for k in order:
            pl.when(exists(*DIRS[k]))(lambda k=k: halo_copy(*item, k).start())

    def wait_halo(*item):
        for k in order:
            dx, dy = DIRS[k]
            pl.when(exists(-dx, -dy))(lambda k=k: halo_copy(*item, k).wait_recv())

    def end_halo(*item):
        for k in order:
            pl.when(exists(*DIRS[k]))(lambda k=k: halo_copy(*item, k).wait_send())

    def around(v, x, start, count):
        lane = lax.broadcasted_iota(jnp.int32, (count, LANES), 1)
        own = pl.ds(start, count)
        centre = [v[x, z, own, :] for z in range(parts)]
        fore = [pltpu.roll(c, 1, 1) for c in centre]
        back = [pltpu.roll(c, LANES - 1, 1) for c in centre]
        out = []
        for z in range(parts):
            near = jnp.where(lane == 0, fore[z - 1] if z > 0 else 0.0, fore[z])
            far = jnp.where(lane == LANES - 1, back[z + 1] if z + 1 < parts else 0.0, back[z])
            beside = v[x - 1, z, own, :] + v[x + 1, z, own, :]
            beside = beside + v[x, z, pl.ds(start - 1, count), :] + v[x, z, pl.ds(start + 1, count), :]
            beside = beside + (near + far)
            out.append(beside)
        return out, centre

    def stencil(v, x, start, count):
        out, centre = around(v, x, start, count)
        own = pl.ds(start, count)
        return [(dmp[x, z, own, :] + (7.0 - MID)) * centre[z] - out[z] for z in range(parts)], centre

    low = jnp.where(y_in[0], 0, PY)
    high = jnp.where(y_in[1], 2 * PY + rows, PY + rows)

    def fold(block):
        return jnp.sum(block.reshape(-1, 8, LANES), axis=0)

    def reach(h):
        return PY - h, -(-(rows + 2 * h) // 8) * 8

    def inside(x, start, count):
        row = lax.broadcasted_iota(jnp.int32, (count, LANES), 0) + start
        ok = jnp.logical_and(row >= low, row < high)
        if PX <= x < PX + half:
            return ok
        return jnp.logical_and(ok, x_in[0] if x < PX else x_in[1])

    def powers(head, work, with_dots=False):
        zero = jnp.zeros((8, LANES), jnp.float32)
        totals = []
        for k in range(1, ITERS + 1):
            h = ITERS - k
            start, count = reach(h)
            prev = head if k == 1 else work[k - 2]
            older = None if k == 1 else head if k == 2 else work[k - 3]
            row = lax.broadcasted_iota(jnp.int32, (count, LANES), 0) + start
            keep = jnp.logical_and(row >= PY, row < PY + rows)
            a, b = zero, zero
            for x in range(PX - h, PX + half + h):
                t, centre = stencil(prev, x, start, count)
                ok = inside(x, start, count)
                for z in range(parts):
                    if k == 1:
                        new = t[z] * (1.0 / HALF)
                    else:
                        new = t[z] * (2.0 / HALF) - older[x, z, pl.ds(start, count), :]
                    if h > 0:
                        new = jnp.where(ok, new, 0.0)
                    work[k - 1][x, z, pl.ds(start, count), :] = new
                    if with_dots and PX <= x < PX + half:
                        square, cross = centre[z] * centre[z], centre[z] * new
                        if h > 0:
                            square, cross = jnp.where(keep, square, 0.0), jnp.where(keep, cross, 0.0)
                        a = a + fold(square)
                        b = b + fold(cross)
            totals += [a, b]
        return totals

    flows = []
    for axes in (("level",), ("gx", "outer", "inner")):
        peers, me, n = [{}], 0, 1
        for a in axes:
            peers = [dict(p, **{a: off}) for p in peers for off in range(extent[a])]
            me, n = me * extent[a] + here[a], n * extent[a]
        peers = [p for p in peers if any(p.values())]
        peers.sort(key=lambda p: -sum(min(off, extent[a] - off) for a, off in p.items()))
        flows.append((peers, me, n))

    def cast(s, turn):
        peers, me, n = flows[s]
        copies = []
        for p in peers:
            at = {a: ring[a][p.get(a, 0)] for a in extent}
            cell = slots[s].at[turn, pl.ds(me, 1), :]
            copies.append(pltpu.make_async_remote_copy(
                src_ref=cell, dst_ref=cell, send_sem=red_send[s].at[turn], recv_sem=red_recv[s].at[turn],
                device_id={"level": at["level"], "gx": at["gx"], "yz": at["outer"] * inner + at["inner"]}, device_id_type=MESH))
        return copies

    def gathered(s, turn):
        bulk = slots[s].at[turn, pl.ds(0, flows[s][2] - 1), :]
        return pltpu.make_async_remote_copy(
            src_ref=bulk, dst_ref=bulk, send_sem=red_send[s].at[turn], recv_sem=red_recv[s].at[turn],
            device_id={"level": 1 - level, "gx": gx, "yz": yz}, device_id_type=MESH)

    def reduce_all(accs, turn, meanwhile):
        n = len(accs)
        size = -(-n // 8) * 8
        eye = lax.broadcasted_iota(jnp.int32, (size, LANES), 0) == lax.broadcasted_iota(jnp.int32, (size, LANES), 1)
        tall = jnp.concatenate([jnp.sum(a, axis=0, keepdims=True) for a in accs]
                               + [jnp.zeros((size - n, LANES), jnp.float32)] * (size > n), axis=0)
        col = jnp.sum(tall, axis=1, keepdims=True)
        line = jnp.sum(jnp.where(eye, col, 0.0), axis=0, keepdims=True)
        for s in range(len(flows)):
            slots[s][turn, pl.ds(flows[s][1], 1), :] = line

            def start(s=s):
                for copy in cast(s, turn):
                    copy.start()

            def finish(s=s):
                gathered(s, turn).wait_recv()

            last = s == len(flows) - 1
            alone = last and turn == STEPS
            pl.when(level == 1)(start) if alone else start()
            if s == 0 and turn == 0:
                meet(ROUNDS)
            if last:
                meanwhile()
            pl.when(level == 1)(finish) if alone else finish()
            line = jnp.sum(slots[s][turn], axis=0, keepdims=True)
        col = jnp.sum(jnp.where(eye, line, 0.0), axis=1, keepdims=True)
        wide = jnp.broadcast_to(col, (size, LANES))
        return [jnp.broadcast_to(wide[k:k + 1, :], (8, LANES)) for k in range(n)]

    def place(part, z):
        return out_ref.at[0, pl.ds(part * half, half), :, slice(z * LANES, (z + 1) * LANES)]

    def across(z):
        return pltpu.make_async_remote_copy(
            src_ref=result.at[:, z], dst_ref=place(1, z), send_sem=p_send.at[z], recv_sem=p_recv.at[z],
            device_id={"level": 0, "gx": gx, "yz": yz}, device_id_type=MESH)

    def upward(k):
        source, target = ((own_c, far_c.at[0:ITERS]), (sums.at[1], far_c.at[ITERS]))[k]
        return pltpu.make_async_remote_copy(
            src_ref=source, dst_ref=target, send_sem=up_send.at[k], recv_sem=up_recv.at[k],
            device_id={"level": 1, "gx": gx, "yz": yz}, device_id_type=MESH)

    def trade():
        @pl.when(level == 0)
        def _():
            for k in range(2):
                upward(k).start()
            for z in range(parts):
                place(0, z)[...] = result[:, z]

        @pl.when(level == 1)
        def _():
            for z in range(parts):
                across(z).start()

    for copy in loads:
        copy.wait()
    for x in range(PX, PX + half):
        for z in range(parts):
            src[x, z, PY:PY + rows, :] = src[x, z, PY:PY + rows, :] - dmp[x, z, PY:PY + rows, :] * p0[x, z, PY:PY + rows, :]
    pl.semaphore_wait(barrier, greeted)
    meet(0)
    starts = ((p0, PX, 0), (src, ITERS, 1), (dmp, ITERS - 1, 2))
    for item in starts:
        send_halo(*item)
    for turn in range(1, ROUNDS):
        meet(turn)
    for item in starts:
        wait_halo(*item)

    start, count = reach(ITERS)
    for x in range(PX - ITERS, PX + half + ITERS):
        t, centre = around(p0, x, start, count)
        ok = inside(x, start, count)
        for z in range(parts):
            r = src[x, z, pl.ds(start, count), :] - (6.0 * centre[z] - t[z])
            first[0, x, z, pl.ds(start, count), :] = jnp.where(ok, r, 0.0)
    accs = powers(first.at[0], (first.at[1], first.at[2], heads_p.at[0]), True)

    pending = list(starts)
    slot = len(starts)
    for turn in range(STEPS + 1):
        with_p, with_c = turn < STEPS, turn > 0
        jobs = []
        for on, head, work in ((with_p, heads_p.at[turn], work_p), (with_p and with_c, heads_c.at[turn - 1], work_c)):
            if on:
                jobs.append(((head, ITERS, slot), work))
                slot += 1
        for item, _ in jobs:
            send_halo(*item)

        def meanwhile(turn=turn, jobs=jobs):
            if turn == STEPS:
                trade()
            for item, work in jobs:
                wait_halo(*item)
                powers(item[0], [work.at[k] for k in range(ITERS)])

        pending += [item for item, _ in jobs]
        dots = reduce_all(accs, turn, meanwhile)
        sets = [cg_coefficients(dots[6 * i:6 * i + 6]) for i in range(len(dots) // 6)]
        if with_p:
            rise_p, step_p = sets[0]
        if with_c:
            rise_c, step_c = sets[-1]
        n_acc = 6 * ((turn + 1 < STEPS) + (turn < STEPS))

        def update(i, accs):
            x = i + PX
            accs = list(accs)
            for z in range(parts):
                for y in range(0, rows, 8):
                    near, wide = pl.ds(y, 8), pl.ds(PY + y, 8)
                    if with_p:
                        if turn == 0:
                            v = [first[j, x, z, wide, :] for j in range(ITERS)]
                        else:
                            v = [own_p[j, i, z, near, :] for j in range(ITERS)]
                        v.append(heads_p[turn, x, z, wide, :])
                        v += [work_p[k, x, z, wide, :] for k in range(ITERS)]
                        before = p0[x, z, wide, :] if turn == 0 else sums[0, i, z, near, :]
                        after = before + combine(rise_p, v)
                        if turn + 1 < STEPS:
                            sums[0, i, z, near, :] = after
                        else:
                            result[i, z, near, :] = after
                        change = shifted(step_p, v)
                    if with_c:
                        u = [own_c[j, i, z, near, :] for j in range(ITERS)]
                        before = p0[x, z, wide, :] if turn == 1 else sums[1, i, z, near, :]
                        sums[1, i, z, near, :] = before + combine(rise_c, u)
                        u.append(heads_c[turn - 1, x, z, wide, :])
                        u += [work_c[k, x, z, wide, :] for k in range(ITERS)]
                    news = []
                    if turn + 1 < STEPS:
                        fresh = [a - b for a, b in zip(v, change)]
                        for j in range(ITERS):
                            own_p[j, i, z, near, :] = fresh[j]
                        heads_p[turn + 1, x, z, wide, :] = fresh[ITERS]
                        news.append(fresh)
                    if turn == 0:
                        ground = v[:ITERS + 1]
                    else:
                        if turn == 1:
                            ground = [first[j, x, z, wide, :] for j in range(ITERS)] + [heads_p[0, x, z, wide, :]]
                        else:
                            ground = [base[j, i, z, near, :] for j in range(ITERS + 1)]
                        ground = [a - b for a, b in zip(ground, shifted(step_c, u))]
                        if turn + 1 < STEPS:
                            for j in range(ITERS + 1):
                                base[j, i, z, near, :] = ground[j]
                    fresh = [a + 0.5 * b for a, b in zip(ground, change)]
                    for j in range(ITERS):
                        own_c[j, i, z, near, :] = fresh[j]
                    heads_c[turn, x, z, wide, :] = fresh[ITERS]
                    news.append(fresh)
                    for f, fresh in enumerate(news):
                        for j in range(ITERS):
                            accs[6 * f + 2 * j] = accs[6 * f + 2 * j] + fresh[j] * fresh[j]
                            accs[6 * f + 2 * j + 1] = accs[6 * f + 2 * j + 1] + fresh[j] * fresh[j + 1]
            return tuple(accs)

        def last(i, carry):
            for z in range(parts):
                for y in range(0, rows, 8):
                    near, lanes = pl.ds(y, 8), slice(z * LANES, (z + 1) * LANES)
                    out_ref[0, half + i, near, lanes] = sums[1, i, z, near, :] + combine(
                        rise_c, [own_c[j, i, z, near, :] for j in range(ITERS)])
                    out_ref[0, i, near, lanes] = far_c[ITERS, i, z, near, :] + combine(
                        rise_c, [far_c[j, i, z, near, :] for j in range(ITERS)])
            return carry

        if turn < STEPS:
            accs = lax.fori_loop(0, half, update, (jnp.zeros((8, LANES), jnp.float32),) * n_acc, unroll=2)
        else:
            @pl.when(level == 1)
            def _():
                for k in range(2):
                    upward(k).wait_recv()
                lax.fori_loop(0, half, last, 0)
    for item in pending:
        end_halo(*item)
    for turn in range(STEPS + 1):
        gathered(0, turn).wait_send()
        if turn < STEPS:
            gathered(1, turn).wait_send()
        else:
            pl.when(level == 1)(lambda turn=turn: gathered(1, turn).wait_send())
    for z in range(parts):
        pl.when(level == 1)(lambda z=z: across(z).wait_send())
        pl.when(level == 0)(lambda z=z: across(z).wait_recv())
    for k in range(2):
        pl.when(level == 0)(lambda k=k: upward(k).wait_send())


def solution(mesh):
    levels, nx, ny = mesh.shape["level"], mesh.shape["gx"], mesh.shape["yz"]

    def per_device(init_field, source, damping):
        deep, rows, wide = init_field.shape
        half, parts = deep // levels, wide // LANES
        padded = (half + 2 * PX, parts, rows + 2 * PY, LANES)
        plain = (half, parts, rows, LANES)
        counts = (levels, nx * ny)
        turns = STEPS + 1
        dma = pltpu.SemaphoreType.DMA
        exchanges = 3 + 2 * STEPS - 1
        vmem = lambda n, shape: pltpu.VMEM((n,) + shape, jnp.float32)
        return pl.pallas_call(
            functools.partial(body, (levels, nx, ny)),
            out_shape=pltpu.VMEM((1, deep, rows, wide), jnp.float32),
            in_specs=[pl.BlockSpec(memory_space=pltpu.HBM)] * 3,
            out_specs=pl.BlockSpec(memory_space=pltpu.VMEM),
            scratch_shapes=[
                pltpu.VMEM(padded, jnp.float32),
                pltpu.VMEM(padded, jnp.float32),
                pltpu.VMEM(padded, jnp.float32),
                vmem(ITERS, padded),
                vmem(STEPS, padded),
                vmem(STEPS, padded),
                vmem(ITERS, plain),
                vmem(ITERS, plain),
                vmem(ITERS + 1, plain),
                vmem(ITERS, padded),
                vmem(ITERS, padded),
                vmem(2, plain),
                pltpu.VMEM(plain, jnp.float32),
                vmem(ITERS + 1, plain),
                [pltpu.VMEM((turns, n, LANES), jnp.float32) for n in counts],
                dma((3, parts)),
                dma((exchanges, 8)),
                dma((exchanges, 8)),
                [dma((turns,)) for n in counts],
                [dma((turns,)) for n in counts],
                dma((parts,)),
                dma((parts,)),
                dma((2,)),
                dma((2,)),
                pltpu.SemaphoreType.REGULAR((ROUNDS,)),
            ],
            compiler_params=pltpu.CompilerParams(has_side_effects=True, collective_id=0),
        )(init_field, source, damping)

    spec = P("gx", "yz", None)
    return jax.shard_map(
        per_device, mesh=mesh, in_specs=(spec, spec, spec),
        out_specs=P("level", "gx", "yz", None), check_vma=False,
    )
```

```python
import functools

import jax
import jax.numpy as jnp
from jax import lax
from jax.experimental import pallas as pl
from jax.experimental.pallas import tpu as pltpu
from jax.sharding import PartitionSpec as P

STEPS = 3
ITERS = 3
ROUNDS = 3
INNER = 4
PX = 4
PY = 8
LANES = 128
MID = 8.025
HALF = 6.975
MESH = pl.DeviceIdType.MESH
DIRS = ((-1, 0), (1, 0), (0, -1), (0, 1), (-1, -1), (-1, 1), (1, -1), (1, 1))


def times_a(c):
    out = [MID * v for v in c] + [jnp.zeros_like(c[0])]
    for k, v in enumerate(c):
        if k == 0:
            out[1] = out[1] + HALF * v
        else:
            out[k + 1] = out[k + 1] + (0.5 * HALF) * v
            out[k - 1] = out[k - 1] + (0.5 * HALF) * v
    return out


def plus(a, b):
    short, long = (a, b) if len(a) < len(b) else (b, a)
    return [x + y for x, y in zip(short, long)] + long[len(short):]


def scaled(s, a):
    return [s * x for x in a]


def cg_coefficients(dots):
    m = [dots[0], dots[1], 2.0 * dots[2] - dots[0], 2.0 * dots[3] - dots[1],
         2.0 * dots[4] - dots[0], 2.0 * dots[5] - dots[1]]

    def inner(a, b):
        total = None
        for i, x in enumerate(a):
            for j, y in enumerate(b):
                term = (x * y) * (0.5 * (m[i + j] + m[abs(i - j)]))
                total = term if total is None else total + term
        return total

    one = jnp.ones_like(m[0])
    resid = [one]
    direction = resid
    image = times_a(resid)
    along = image
    norm_now = m[0]
    alpha = norm_now / inner(resid, image)
    answer = None
    for step in range(ITERS):
        move = scaled(alpha, direction)
        answer = move if answer is None else plus(answer, move)
        if step + 1 < ITERS:
            resid = plus(resid, scaled(-alpha, along))
            image = times_a(resid)
            norm_next = inner(resid, resid)
            product = inner(resid, image)
            ratio = norm_next / norm_now
            alpha = norm_next / (product - ratio * norm_next / alpha)
            direction = plus(resid, scaled(ratio, direction))
            along = plus(image, scaled(ratio, along))
            norm_now = norm_next
    change = plus(times_a(answer), scaled(-1.0, answer))
    return answer, change


def shifted(c, v):
    t, w = v[:ITERS + 1], v[ITERS + 1:]
    one, two = 0.5 * c[1], 0.5 * c[2]
    even, odd, gap = t[0] + t[2], t[1] + t[3], t[0] - t[2]
    return [
        c[0] * t[0] + c[1] * t[1] + (c[2] * t[2] + c[3] * t[3]),
        c[0] * t[1] + one * even + (two * odd + c[3] * w[0]),
        c[0] * t[2] + one * odd + (two * gap + c[2] * w[0]) + c[3] * w[1],
    ]


def lifted(c, t, w):
    return c[0] * t + c[1] * w[0] + (c[2] * w[1] + c[3] * w[2])


def combine(c, v):
    total = None
    for a, b in zip(c, v):
        total = a * b if total is None else total + a * b
    return total


def body(sizes, init_ref, source_ref, damp_ref, out_ref, p0, src, dmp, first, heads_p, heads_c, own_p, own_c,
         base, work_p, work_c, sums, result, far_c, slots, in_sem, send_sem, recv_sem, red_send, red_recv, p_send, p_recv, up_send, up_recv,
         met):
    levels, nx, ny = sizes
    half = own_p.shape[1]
    parts = p0.shape[1]
    rows = own_p.shape[3]
    level, gx, yz = lax.axis_index("level"), lax.axis_index("gx"), lax.axis_index("yz")
    xpos = gx * levels + level
    xcount = nx * levels
    x_in = (xpos > 0, xpos < xcount - 1)
    y_in = (yz > 0, yz < ny - 1)

    def exists(dx, dy):
        ok = None
        for d, at, count in ((dx, xpos, xcount), (dy, yz, ny)):
            if d != 0:
                c = at + d >= 0 if d < 0 else at + d < count
                ok = c if ok is None else jnp.logical_and(ok, c)
        return ok

    def beside(dx, dy):
        to = xpos + dx
        return {"level": lax.rem(to + xcount, levels), "gx": lax.div(to + xcount, levels) - nx, "yz": yz + dy}

    mine = pl.ds(level * half, half)
    loads = []
    for i, (ref, buf) in enumerate(((init_ref, p0), (source_ref, src), (damp_ref, dmp))):
        for z in range(parts):
            copy = pltpu.make_async_copy(ref.at[mine, :, slice(z * LANES, (z + 1) * LANES)],
                                         buf.at[PX:PX + half, z, PY:PY + rows, :], in_sem.at[i, z])
            copy.start()
            loads.append(copy)

    def signal_all(sem, steps):
        count = 0
        for dx, dy in steps:
            ok = exists(dx, dy)
            count = count + jnp.where(ok, 1, 0)

            @pl.when(ok)
            def _(dx=dx, dy=dy):
                pl.semaphore_signal(sem, inc=1, device_id=beside(dx, dy), device_id_type=MESH)
        return count

    inner = INNER if ny % INNER == 0 else 1
    extent = {"level": levels, "gx": nx, "outer": ny // inner, "inner": inner}
    here = {"level": level, "gx": gx, "outer": lax.div(yz, inner), "inner": lax.rem(yz, inner)}
    ring = {a: [here[a]] + [lax.rem(here[a] + off, n) for off in range(1, n)] for a, n in extent.items()}
    deep = extent["outer"]
    rounds = ([(0, k) for k in range(1, inner)] + [(1, 0), (deep - 1, 0)],
              [(1, 0), (2, 0), (deep - 2, 0), (deep - 1, 0)],
              [(k, 0) for k in range(3, deep - 2)])

    def call(sem, steps):
        for far, near in steps:
            pl.semaphore_signal(sem, inc=1, device_id_type=MESH, device_id={
                "level": level, "gx": gx, "yz": ring["outer"][far] * inner + ring["inner"][near]})

    def meet(turn):
        if turn > 0:
            pl.semaphore_wait(met.at[turn - 1], len(rounds[turn - 1]))
        if turn < ROUNDS:
            call(met.at[turn], rounds[turn])

    barrier = pltpu.get_barrier_semaphore()
    greeted = signal_all(barrier, DIRS + tuple((d, 0) for d in range(1 - xcount, xcount) if abs(d) > 1)) + len(rounds[0])
    call(barrier, rounds[0])

    zero_x = jnp.zeros((PX,) + tuple(p0.shape[1:]), jnp.float32)
    zero_y = jnp.zeros((p0.shape[0], parts, PY, LANES), jnp.float32)
    for buf in [p0] + [heads_p.at[n] for n in range(STEPS)] + [heads_c.at[n] for n in range(STEPS - 1)]:
        @pl.when(jnp.logical_not(x_in[0]))
        def _(buf=buf):
            buf[0:PX] = zero_x

        @pl.when(jnp.logical_not(x_in[1]))
        def _(buf=buf):
            buf[PX + half:] = zero_x

        @pl.when(jnp.logical_not(y_in[0]))
        def _(buf=buf):
            buf[:, :, 0:PY, :] = zero_y

        @pl.when(jnp.logical_not(y_in[1]))
        def _(buf=buf):
            buf[:, :, PY + rows:, :] = zero_y

    def halo_copy(buf, width, slot, k):
        dx, dy = DIRS[k]
        w = width if 0 in (dx, dy) else width - 1

        def spans(d, pad, size):
            if d == 0:
                return slice(pad, pad + size), slice(pad, pad + size)
            if d < 0:
                return slice(pad, pad + w), slice(pad + size, pad + size + w)
            return slice(pad + size - w, pad + size), slice(pad - w, pad)

        sx, tx = spans(dx, PX, half)
        sy, ty = spans(dy, PY, rows)
        return pltpu.make_async_remote_copy(
            src_ref=buf.at[sx, :, sy, :], dst_ref=buf.at[tx, :, ty, :],
            send_sem=send_sem.at[slot, k], recv_sem=recv_sem.at[slot, k],
            device_id=beside(dx, dy), device_id_type=MESH,
        )

    order = (2, 3, 4, 5, 6, 7, 0, 1)

    def send_halo(*item):
        for k in order:
            pl.when(exists(*DIRS[k]))(lambda k=k: halo_copy(*item, k).start())

    def wait_halo(*item):
        for k in order:
            dx, dy = DIRS[k]
            pl.when(exists(-dx, -dy))(lambda k=k: halo_copy(*item, k).wait_recv())

    def end_halo(*item):
        for k in order:
            pl.when(exists(*DIRS[k]))(lambda k=k: halo_copy(*item, k).wait_send())

    def around(v, x, start, count):
        lane = lax.broadcasted_iota(jnp.int32, (count, LANES), 1)
        own = pl.ds(start, count)
        centre = [v[x, z, own, :] for z in range(parts)]
        fore = [pltpu.roll(c, 1, 1) for c in centre]
        back = [pltpu.roll(c, LANES - 1, 1) for c in centre]
        out = []
        for z in range(parts):
            near = jnp.where(lane == 0, fore[z - 1] if z > 0 else 0.0, fore[z])
            far = jnp.where(lane == LANES - 1, back[z + 1] if z + 1 < parts else 0.0, back[z])
            beside = v[x - 1, z, own, :] + v[x + 1, z, own, :]
            beside = beside + v[x, z, pl.ds(start - 1, count), :] + v[x, z, pl.ds(start + 1, count), :]
            beside = beside + (near + far)
            out.append(beside)
        return out, centre

    def stencil(v, x, start, count):
        out, centre = around(v, x, start, count)
        own = pl.ds(start, count)
        return [(dmp[x, z, own, :] + (7.0 - MID)) * centre[z] - out[z] for z in range(parts)], centre

    low = jnp.where(y_in[0], 0, PY)
    high = jnp.where(y_in[1], 2 * PY + rows, PY + rows)

    def fold(block):
        return jnp.sum(block.reshape(-1, 8, LANES), axis=0)

    def reach(h):
        return PY - h, -(-(rows + 2 * h) // 8) * 8

    def inside(x, start, count):
        row = lax.broadcasted_iota(jnp.int32, (count, LANES), 0) + start
        ok = jnp.logical_and(row >= low, row < high)
        if PX <= x < PX + half:
            return ok
        return jnp.logical_and(ok, x_in[0] if x < PX else x_in[1])

    def powers(head, work, with_dots=False):
        zero = jnp.zeros((8, LANES), jnp.float32)
        totals = []
        for k in range(1, ITERS + 1):
            h = ITERS - k
            start, count = reach(h)
            prev = head if k == 1 else work[k - 2]
            older = None if k == 1 else head if k == 2 else work[k - 3]
            row = lax.broadcasted_iota(jnp.int32, (count, LANES), 0) + start
            keep = jnp.logical_and(row >= PY, row < PY + rows)
            a, b = zero, zero
            for x in range(PX - h, PX + half + h):
                t, centre = stencil(prev, x, start, count)
                ok = inside(x, start, count)
                for z in range(parts):
                    if k == 1:
                        new = t[z] * (1.0 / HALF)
                    else:
                        new = t[z] * (2.0 / HALF) - older[x, z, pl.ds(start, count), :]
                    if h > 0:
                        new = jnp.where(ok, new, 0.0)
                    work[k - 1][x, z, pl.ds(start, count), :] = new
                    if with_dots and PX <= x < PX + half:
                        square, cross = centre[z] * centre[z], centre[z] * new
                        if h > 0:
                            square, cross = jnp.where(keep, square, 0.0), jnp.where(keep, cross, 0.0)
                        a = a + fold(square)
                        b = b + fold(cross)
            totals += [a, b]
        return totals

    flows = []
    for axes in (("level",), ("gx", "outer", "inner")):
        peers, me, n = [{}], 0, 1
        for a in axes:
            peers = [dict(p, **{a: off}) for p in peers for off in range(extent[a])]
            me, n = me * extent[a] + here[a], n * extent[a]
        peers = [p for p in peers if any(p.values())]
        peers.sort(key=lambda p: -sum(min(off, extent[a] - off) for a, off in p.items()))
        flows.append((peers, me, n))

    def cast(s, turn):
        peers, me, n = flows[s]
        copies = []
        for p in peers:
            at = {a: ring[a][p.get(a, 0)] for a in extent}
            cell = slots[s].at[turn, pl.ds(me, 1), :]
            copies.append(pltpu.make_async_remote_copy(
                src_ref=cell, dst_ref=cell, send_sem=red_send[s].at[turn], recv_sem=red_recv[s].at[turn],
                device_id={"level": at["level"], "gx": at["gx"], "yz": at["outer"] * inner + at["inner"]}, device_id_type=MESH))
        return copies

    def gathered(s, turn):
        bulk = slots[s].at[turn, pl.ds(0, flows[s][2] - 1), :]
        return pltpu.make_async_remote_copy(
            src_ref=bulk, dst_ref=bulk, send_sem=red_send[s].at[turn], recv_sem=red_recv[s].at[turn],
            device_id={"level": 1 - level, "gx": gx, "yz": yz}, device_id_type=MESH)

    def reduce_all(accs, turn, meanwhile):
        n = len(accs)
        size = -(-n // 8) * 8
        eye = lax.broadcasted_iota(jnp.int32, (size, LANES), 0) == lax.broadcasted_iota(jnp.int32, (size, LANES), 1)
        tall = jnp.concatenate([jnp.sum(a, axis=0, keepdims=True) for a in accs]
                               + [jnp.zeros((size - n, LANES), jnp.float32)] * (size > n), axis=0)
        col = jnp.sum(tall, axis=1, keepdims=True)
        line = jnp.sum(jnp.where(eye, col, 0.0), axis=0, keepdims=True)
        for s in range(len(flows)):
            slots[s][turn, pl.ds(flows[s][1], 1), :] = line

            def start(s=s):
                for copy in cast(s, turn):
                    copy.start()

            def finish(s=s):
                gathered(s, turn).wait_recv()

            last = s == len(flows) - 1
            alone = last and turn == STEPS
            pl.when(level == 1)(start) if alone else start()
            if s == 0 and turn == 0:
                meet(ROUNDS)
            if last:
                meanwhile()
            pl.when(level == 1)(finish) if alone else finish()
            line = jnp.sum(slots[s][turn], axis=0, keepdims=True)
        col = jnp.sum(jnp.where(eye, line, 0.0), axis=1, keepdims=True)
        wide = jnp.broadcast_to(col, (size, LANES))
        return [jnp.broadcast_to(wide[k:k + 1, :], (8, LANES)) for k in range(n)]

    def place(part, z):
        return out_ref.at[0, pl.ds(part * half, half), :, slice(z * LANES, (z + 1) * LANES)]

    def across(z):
        return pltpu.make_async_remote_copy(
            src_ref=result.at[:, z], dst_ref=place(1, z), send_sem=p_send.at[z], recv_sem=p_recv.at[z],
            device_id={"level": 0, "gx": gx, "yz": yz}, device_id_type=MESH)

    def upward(k):
        source, target = ((own_c, far_c.at[0:ITERS]), (sums.at[1], far_c.at[ITERS]))[k]
        return pltpu.make_async_remote_copy(
            src_ref=source, dst_ref=target, send_sem=up_send.at[k], recv_sem=up_recv.at[k],
            device_id={"level": 1, "gx": gx, "yz": yz}, device_id_type=MESH)

    def trade():
        @pl.when(level == 0)
        def _():
            for k in range(2):
                upward(k).start()
            for z in range(parts):
                place(0, z)[...] = result[:, z]

        @pl.when(level == 1)
        def _():
            for z in range(parts):
                across(z).start()

    for copy in loads:
        copy.wait()
    for x in range(PX, PX + half):
        for z in range(parts):
            src[x, z, PY:PY + rows, :] = src[x, z, PY:PY + rows, :] - dmp[x, z, PY:PY + rows, :] * p0[x, z, PY:PY + rows, :]
    pl.semaphore_wait(barrier, greeted)
    meet(0)
    starts = ((p0, PX, 0), (src, ITERS, 1), (dmp, ITERS - 1, 2))
    for item in starts:
        send_halo(*item)
    for turn in range(1, ROUNDS):
        meet(turn)
    for item in starts[:2]:
        wait_halo(*item)

    start, count = reach(ITERS)
    for x in range(PX - ITERS, PX + half + ITERS):
        t, centre = around(p0, x, start, count)
        ok = inside(x, start, count)
        for z in range(parts):
            r = src[x, z, pl.ds(start, count), :] - (6.0 * centre[z] - t[z])
            first[0, x, z, pl.ds(start, count), :] = jnp.where(ok, r, 0.0)
    wait_halo(*starts[2])
    accs = powers(first.at[0], (first.at[1], first.at[2], heads_p.at[0]), True)

    pending = list(starts)
    slot = len(starts)
    plan = []
    for turn in range(STEPS + 1):
        jobs = []
        for on, heads, at, work in ((turn < STEPS, heads_p, turn, work_p), (0 < turn < STEPS, heads_c, turn - 1, work_c)):
            if on:
                jobs.append(((heads.at[at], ITERS, slot), work))
                slot += 1
        plan.append(jobs)
    for item, _ in plan[0]:
        send_halo(*item)
    for turn in range(STEPS + 1):
        with_p, with_c = turn < STEPS, turn > 0
        jobs = plan[turn]

        def meanwhile(turn=turn, jobs=jobs):
            if turn == STEPS:
                trade()
            for item, work in jobs:
                wait_halo(*item)
                powers(item[0], [work.at[k] for k in range(ITERS)])

        pending += [item for item, _ in jobs]
        dots = reduce_all(accs, turn, meanwhile)
        sets = [cg_coefficients(dots[6 * i:6 * i + 6]) for i in range(len(dots) // 6)]
        if with_p:
            rise_p, step_p = sets[0]
        if with_c:
            rise_c, step_c = sets[-1]
        n_acc = 6 * ((turn + 1 < STEPS) + (turn < STEPS))

        def top(x, i, z, near, wide):
            before = heads_p[turn, x, z, wide, :]
            change = lifted(step_p, before, [work_p[k, x, z, wide, :] for k in range(ITERS)])
            fresh = []
            if turn + 1 < STEPS:
                fresh.append(before - change)
                heads_p[turn + 1, x, z, wide, :] = fresh[0]
            ground = before
            if with_c:
                ground = heads_p[0, x, z, wide, :] if turn == 1 else base[ITERS, i, z, near, :]
                ground = ground - lifted(step_c, heads_c[turn - 1, x, z, wide, :],
                                         [work_c[k, x, z, wide, :] for k in range(ITERS)])
                if turn + 1 < STEPS:
                    base[ITERS, i, z, near, :] = ground
            fresh.append(ground + 0.5 * change)
            heads_c[turn, x, z, wide, :] = fresh[-1]
            return fresh

        def lead(i, carry):
            for z in range(parts):
                for y in range(0, rows, 8):
                    top(i + PX, i, z, pl.ds(y, 8), pl.ds(PY + y, 8))
            return carry

        def update(i, accs):
            x = i + PX
            accs = list(accs)
            for z in range(parts):
                for y in range(0, rows, 8):
                    near, wide = pl.ds(y, 8), pl.ds(PY + y, 8)
                    if with_p:
                        if turn == 0:
                            v = [first[j, x, z, wide, :] for j in range(ITERS)]
                        else:
                            v = [own_p[j, i, z, near, :] for j in range(ITERS)]
                        v.append(heads_p[turn, x, z, wide, :])
                        v += [work_p[k, x, z, wide, :] for k in range(ITERS)]
                        before = p0[x, z, wide, :] if turn == 0 else sums[0, i, z, near, :]
                        after = before + combine(rise_p, v)
                        if turn + 1 < STEPS:
                            sums[0, i, z, near, :] = after
                        else:
                            result[i, z, near, :] = after
                        change = shifted(step_p, v)
                    if with_c:
                        u = [own_c[j, i, z, near, :] for j in range(ITERS)]
                        before = p0[x, z, wide, :] if turn == 1 else sums[1, i, z, near, :]
                        sums[1, i, z, near, :] = before + combine(rise_c, u)
                        u.append(heads_c[turn - 1, x, z, wide, :])
                        u += [work_c[k, x, z, wide, :] for k in range(ITERS)]
                    if turn + 1 < STEPS:
                        tops = [heads_p[turn + 1, x, z, wide, :], heads_c[turn, x, z, wide, :]]
                    else:
                        tops = top(x, i, z, near, wide)
                    news = []
                    if turn + 1 < STEPS:
                        fresh = [a - b for a, b in zip(v, change)]
                        for j in range(ITERS):
                            own_p[j, i, z, near, :] = fresh[j]
                        news.append(fresh)
                    if turn == 0:
                        ground = v[:ITERS]
                    else:
                        if turn == 1:
                            ground = [first[j, x, z, wide, :] for j in range(ITERS)]
                        else:
                            ground = [base[j, i, z, near, :] for j in range(ITERS)]
                        ground = [a - b for a, b in zip(ground, shifted(step_c, u))]
                        if turn + 1 < STEPS:
                            for j in range(ITERS):
                                base[j, i, z, near, :] = ground[j]
                    fresh = [a + 0.5 * b for a, b in zip(ground, change)]
                    for j in range(ITERS):
                        own_c[j, i, z, near, :] = fresh[j]
                    news.append(fresh)
                    news = [own + [far] for own, far in zip(news, tops)]
                    for f, fresh in enumerate(news):
                        for j in range(ITERS):
                            accs[6 * f + 2 * j] = accs[6 * f + 2 * j] + fresh[j] * fresh[j]
                            accs[6 * f + 2 * j + 1] = accs[6 * f + 2 * j + 1] + fresh[j] * fresh[j + 1]
            return tuple(accs)

        def last(i, carry):
            for z in range(parts):
                for y in range(0, rows, 8):
                    near, lanes = pl.ds(y, 8), slice(z * LANES, (z + 1) * LANES)
                    out_ref[0, half + i, near, lanes] = sums[1, i, z, near, :] + combine(
                        rise_c, [own_c[j, i, z, near, :] for j in range(ITERS)])
                    out_ref[0, i, near, lanes] = far_c[ITERS, i, z, near, :] + combine(
                        rise_c, [far_c[j, i, z, near, :] for j in range(ITERS)])
            return carry

        if turn + 1 < STEPS:
            lax.fori_loop(0, half, lead, 0, unroll=2)
            for item, _ in plan[turn + 1]:
                send_halo(*item)
        if turn < STEPS:
            accs = lax.fori_loop(0, half, update, (jnp.zeros((8, LANES), jnp.float32),) * n_acc, unroll=2)
        else:
            @pl.when(level == 1)
            def _():
                for k in range(2):
                    upward(k).wait_recv()
                lax.fori_loop(0, half, last, 0)
    for item in pending:
        end_halo(*item)
    for turn in range(STEPS + 1):
        gathered(0, turn).wait_send()
        if turn < STEPS:
            gathered(1, turn).wait_send()
        else:
            pl.when(level == 1)(lambda turn=turn: gathered(1, turn).wait_send())
    for z in range(parts):
        pl.when(level == 1)(lambda z=z: across(z).wait_send())
        pl.when(level == 0)(lambda z=z: across(z).wait_recv())
    for k in range(2):
        pl.when(level == 0)(lambda k=k: upward(k).wait_send())


def solution(mesh):
    levels, nx, ny = mesh.shape["level"], mesh.shape["gx"], mesh.shape["yz"]

    def per_device(init_field, source, damping):
        deep, rows, wide = init_field.shape
        half, parts = deep // levels, wide // LANES
        padded = (half + 2 * PX, parts, rows + 2 * PY, LANES)
        plain = (half, parts, rows, LANES)
        counts = (levels, nx * ny)
        turns = STEPS + 1
        dma = pltpu.SemaphoreType.DMA
        exchanges = 3 + 2 * STEPS - 1
        vmem = lambda n, shape: pltpu.VMEM((n,) + shape, jnp.float32)
        return pl.pallas_call(
            functools.partial(body, (levels, nx, ny)),
            out_shape=pltpu.VMEM((1, deep, rows, wide), jnp.float32),
            in_specs=[pl.BlockSpec(memory_space=pltpu.HBM)] * 3,
            out_specs=pl.BlockSpec(memory_space=pltpu.VMEM),
            scratch_shapes=[
                pltpu.VMEM(padded, jnp.float32),
                pltpu.VMEM(padded, jnp.float32),
                pltpu.VMEM(padded, jnp.float32),
                vmem(ITERS, padded),
                vmem(STEPS, padded),
                vmem(STEPS, padded),
                vmem(ITERS, plain),
                vmem(ITERS, plain),
                vmem(ITERS + 1, plain),
                vmem(ITERS, padded),
                vmem(ITERS, padded),
                vmem(2, plain),
                pltpu.VMEM(plain, jnp.float32),
                vmem(ITERS + 1, plain),
                [pltpu.VMEM((turns, n, LANES), jnp.float32) for n in counts],
                dma((3, parts)),
                dma((exchanges, 8)),
                dma((exchanges, 8)),
                [dma((turns,)) for n in counts],
                [dma((turns,)) for n in counts],
                dma((parts,)),
                dma((parts,)),
                dma((2,)),
                dma((2,)),
                pltpu.SemaphoreType.REGULAR((ROUNDS,)),
            ],
            compiler_params=pltpu.CompilerParams(has_side_effects=True, collective_id=0),
        )(init_field, source, damping)

    spec = P("gx", "yz", None)
    return jax.shard_map(
        per_device, mesh=mesh, in_specs=(spec, spec, spec),
        out_specs=P("level", "gx", "yz", None), check_vma=False,
    )
```

```python
import functools

import jax
import jax.numpy as jnp
from jax import lax
from jax.experimental import pallas as pl
from jax.experimental.pallas import tpu as pltpu
from jax.sharding import PartitionSpec as P

STEPS = 3
ITERS = 3
ROUNDS = 3
INNER = 4
PX = 4
PY = 8
LANES = 128
MID = 8.025
HALF = 6.975
MESH = pl.DeviceIdType.MESH
DIRS = ((-1, 0), (1, 0), (0, -1), (0, 1), (-1, -1), (-1, 1), (1, -1), (1, 1))


def times_a(c):
    out = [MID * v for v in c] + [jnp.zeros_like(c[0])]
    for k, v in enumerate(c):
        if k == 0:
            out[1] = out[1] + HALF * v
        else:
            out[k + 1] = out[k + 1] + (0.5 * HALF) * v
            out[k - 1] = out[k - 1] + (0.5 * HALF) * v
    return out


def plus(a, b):
    short, long = (a, b) if len(a) < len(b) else (b, a)
    return [x + y for x, y in zip(short, long)] + long[len(short):]


def scaled(s, a):
    return [s * x for x in a]


def cg_coefficients(dots):
    m = [dots[0], dots[1], 2.0 * dots[2] - dots[0], 2.0 * dots[3] - dots[1],
         2.0 * dots[4] - dots[0], 2.0 * dots[5] - dots[1]]

    def inner(a, b):
        total = None
        for i, x in enumerate(a):
            for j, y in enumerate(b):
                term = (x * y) * (0.5 * (m[i + j] + m[abs(i - j)]))
                total = term if total is None else total + term
        return total

    one = jnp.ones_like(m[0])
    resid = [one]
    direction = resid
    image = times_a(resid)
    along = image
    norm_now = m[0]
    alpha = norm_now / inner(resid, image)
    answer = None
    for step in range(ITERS):
        move = scaled(alpha, direction)
        answer = move if answer is None else plus(answer, move)
        if step + 1 < ITERS:
            resid = plus(resid, scaled(-alpha, along))
            image = times_a(resid)
            norm_next = inner(resid, resid)
            product = inner(resid, image)
            ratio = norm_next / norm_now
            alpha = norm_next / (product - ratio * norm_next / alpha)
            direction = plus(resid, scaled(ratio, direction))
            along = plus(image, scaled(ratio, along))
            norm_now = norm_next
    change = plus(times_a(answer), scaled(-1.0, answer))
    return answer, change


def shifted(c, v):
    t, w = v[:ITERS + 1], v[ITERS + 1:]
    one, two = 0.5 * c[1], 0.5 * c[2]
    even, odd, gap = t[0] + t[2], t[1] + t[3], t[0] - t[2]
    return [
        c[0] * t[0] + c[1] * t[1] + (c[2] * t[2] + c[3] * t[3]),
        c[0] * t[1] + one * even + (two * odd + c[3] * w[0]),
        c[0] * t[2] + one * odd + (two * gap + c[2] * w[0]) + c[3] * w[1],
    ]


def lifted(c, t, w):
    return c[0] * t + c[1] * w[0] + (c[2] * w[1] + c[3] * w[2])


def combine(c, v):
    total = None
    for a, b in zip(c, v):
        total = a * b if total is None else total + a * b
    return total


def body(sizes, init_ref, source_ref, damp_ref, out_ref, p0, src, dmp, first, heads_p, heads_c, own_p, own_c,
         base, work_p, work_c, sums, result, far_c, slots, in_sem, send_sem, recv_sem, red_send, red_recv, p_send, p_recv, up_send, up_recv,
         met):
    levels, nx, ny = sizes
    half = own_p.shape[1]
    parts = p0.shape[1]
    rows = own_p.shape[3]
    level, gx, yz = lax.axis_index("level"), lax.axis_index("gx"), lax.axis_index("yz")
    xpos = gx * levels + level
    xcount = nx * levels
    x_in = (xpos > 0, xpos < xcount - 1)
    y_in = (yz > 0, yz < ny - 1)

    def exists(dx, dy):
        ok = None
        for d, at, count in ((dx, xpos, xcount), (dy, yz, ny)):
            if d != 0:
                c = at + d >= 0 if d < 0 else at + d < count
                ok = c if ok is None else jnp.logical_and(ok, c)
        return ok

    def beside(dx, dy):
        to = xpos + dx
        return {"level": lax.rem(to + xcount, levels), "gx": lax.div(to + xcount, levels) - nx, "yz": yz + dy}

    mine = pl.ds(level * half, half)
    loads = []
    for i, (ref, buf) in enumerate(((init_ref, p0), (source_ref, src), (damp_ref, dmp))):
        for z in range(parts):
            copy = pltpu.make_async_copy(ref.at[mine, :, slice(z * LANES, (z + 1) * LANES)],
                                         buf.at[PX:PX + half, z, PY:PY + rows, :], in_sem.at[i, z])
            copy.start()
            loads.append(copy)

    def signal_all(sem, steps):
        count = 0
        for dx, dy in steps:
            ok = exists(dx, dy)
            count = count + jnp.where(ok, 1, 0)

            @pl.when(ok)
            def _(dx=dx, dy=dy):
                pl.semaphore_signal(sem, inc=1, device_id=beside(dx, dy), device_id_type=MESH)
        return count

    inner = INNER if ny % INNER == 0 else 1
    extent = {"level": levels, "gx": nx, "outer": ny // inner, "inner": inner}
    here = {"level": level, "gx": gx, "outer": lax.div(yz, inner), "inner": lax.rem(yz, inner)}
    ring = {a: [here[a]] + [lax.rem(here[a] + off, n) for off in range(1, n)] for a, n in extent.items()}
    deep = extent["outer"]
    rounds = ([(0, k) for k in range(1, inner)] + [(1, 0), (deep - 1, 0)],
              [(1, 0), (2, 0), (deep - 2, 0), (deep - 1, 0)],
              [(k, 0) for k in range(3, deep - 2)])

    def call(sem, steps):
        for far, near in steps:
            pl.semaphore_signal(sem, inc=1, device_id_type=MESH, device_id={
                "level": level, "gx": gx, "yz": ring["outer"][far] * inner + ring["inner"][near]})

    def meet(turn):
        if turn > 0:
            pl.semaphore_wait(met.at[turn - 1], len(rounds[turn - 1]))
        if turn < ROUNDS:
            call(met.at[turn], rounds[turn])

    barrier = pltpu.get_barrier_semaphore()
    greeted = signal_all(barrier, DIRS + tuple((d, 0) for d in range(1 - xcount, xcount) if abs(d) > 1)) + len(rounds[0])
    call(barrier, rounds[0])

    zero_x = jnp.zeros((PX,) + tuple(p0.shape[1:]), jnp.float32)
    zero_y = jnp.zeros((p0.shape[0], parts, PY, LANES), jnp.float32)
    for buf in [p0] + [heads_p.at[n] for n in range(STEPS)] + [heads_c.at[n] for n in range(STEPS - 1)]:
        @pl.when(jnp.logical_not(x_in[0]))
        def _(buf=buf):
            buf[0:PX] = zero_x

        @pl.when(jnp.logical_not(x_in[1]))
        def _(buf=buf):
            buf[PX + half:] = zero_x

        @pl.when(jnp.logical_not(y_in[0]))
        def _(buf=buf):
            buf[:, :, 0:PY, :] = zero_y

        @pl.when(jnp.logical_not(y_in[1]))
        def _(buf=buf):
            buf[:, :, PY + rows:, :] = zero_y

    def halo_copy(buf, width, slot, k):
        dx, dy = DIRS[k]
        w = width if 0 in (dx, dy) else width - 1

        def spans(d, pad, size):
            if d == 0:
                return slice(pad, pad + size), slice(pad, pad + size)
            if d < 0:
                return slice(pad, pad + w), slice(pad + size, pad + size + w)
            return slice(pad + size - w, pad + size), slice(pad - w, pad)

        sx, tx = spans(dx, PX, half)
        sy, ty = spans(dy, PY, rows)
        return pltpu.make_async_remote_copy(
            src_ref=buf.at[sx, :, sy, :], dst_ref=buf.at[tx, :, ty, :],
            send_sem=send_sem.at[slot, k], recv_sem=recv_sem.at[slot, k],
            device_id=beside(dx, dy), device_id_type=MESH,
        )

    order = (2, 3, 4, 5, 6, 7, 0, 1)

    def send_halo(*item):
        for k in order:
            pl.when(exists(*DIRS[k]))(lambda k=k: halo_copy(*item, k).start())

    def wait_halo(*item):
        for k in order:
            dx, dy = DIRS[k]
            pl.when(exists(-dx, -dy))(lambda k=k: halo_copy(*item, k).wait_recv())

    def end_halo(*item):
        for k in order:
            pl.when(exists(*DIRS[k]))(lambda k=k: halo_copy(*item, k).wait_send())

    def around(v, x, start, count):
        lane = lax.broadcasted_iota(jnp.int32, (count, LANES), 1)
        own = pl.ds(start, count)
        centre = [v[x, z, own, :] for z in range(parts)]
        fore = [pltpu.roll(c, 1, 1) for c in centre]
        back = [pltpu.roll(c, LANES - 1, 1) for c in centre]
        out = []
        for z in range(parts):
            near = jnp.where(lane == 0, fore[z - 1] if z > 0 else 0.0, fore[z])
            far = jnp.where(lane == LANES - 1, back[z + 1] if z + 1 < parts else 0.0, back[z])
            beside = v[x - 1, z, own, :] + v[x + 1, z, own, :]
            beside = beside + v[x, z, pl.ds(start - 1, count), :] + v[x, z, pl.ds(start + 1, count), :]
            beside = beside + (near + far)
            out.append(beside)
        return out, centre

    def stencil(v, x, start, count):
        out, centre = around(v, x, start, count)
        own = pl.ds(start, count)
        return [(dmp[x, z, own, :] + (7.0 - MID)) * centre[z] - out[z] for z in range(parts)], centre

    low = jnp.where(y_in[0], 0, PY)
    high = jnp.where(y_in[1], 2 * PY + rows, PY + rows)

    def fold(block):
        return jnp.sum(block.reshape(-1, 8, LANES), axis=0)

    def reach(h):
        return PY - h, -(-(rows + 2 * h) // 8) * 8

    def inside(x, start, count):
        row = lax.broadcasted_iota(jnp.int32, (count, LANES), 0) + start
        ok = jnp.logical_and(row >= low, row < high)
        if PX <= x < PX + half:
            return ok
        return jnp.logical_and(ok, x_in[0] if x < PX else x_in[1])

    def powers(head, work, with_dots=False):
        zero = jnp.zeros((8, LANES), jnp.float32)
        totals = []
        for k in range(1, ITERS + 1):
            h = ITERS - k
            start, count = reach(h)
            prev = head if k == 1 else work[k - 2]
            older = None if k == 1 else head if k == 2 else work[k - 3]
            row = lax.broadcasted_iota(jnp.int32, (count, LANES), 0) + start
            keep = jnp.logical_and(row >= PY, row < PY + rows)
            a, b = zero, zero
            for x in range(PX - h, PX + half + h):
                t, centre = stencil(prev, x, start, count)
                ok = inside(x, start, count)
                for z in range(parts):
                    if k == 1:
                        new = t[z] * (1.0 / HALF)
                    else:
                        new = t[z] * (2.0 / HALF) - older[x, z, pl.ds(start, count), :]
                    if h > 0:
                        new = jnp.where(ok, new, 0.0)
                    work[k - 1][x, z, pl.ds(start, count), :] = new
                    if with_dots and PX <= x < PX + half:
                        square, cross = centre[z] * centre[z], centre[z] * new
                        if h > 0:
                            square, cross = jnp.where(keep, square, 0.0), jnp.where(keep, cross, 0.0)
                        a = a + fold(square)
                        b = b + fold(cross)
            totals += [a, b]
        return totals

    flows = []
    for axes in (("level",), ("gx", "outer", "inner")):
        peers, me, n = [{}], 0, 1
        for a in axes:
            peers = [dict(p, **{a: off}) for p in peers for off in range(extent[a])]
            me, n = me * extent[a] + here[a], n * extent[a]
        peers = [p for p in peers if any(p.values())]
        peers.sort(key=lambda p: -sum(min(off, extent[a] - off) for a, off in p.items()))
        flows.append((peers, me, n))

    def cast(s, turn):
        peers, me, n = flows[s]
        copies = []
        for p in peers:
            at = {a: ring[a][p.get(a, 0)] for a in extent}
            cell = slots[s].at[turn, pl.ds(me, 1), :]
            copies.append(pltpu.make_async_remote_copy(
                src_ref=cell, dst_ref=cell, send_sem=red_send[s].at[turn], recv_sem=red_recv[s].at[turn],
                device_id={"level": at["level"], "gx": at["gx"], "yz": at["outer"] * inner + at["inner"]}, device_id_type=MESH))
        return copies

    def gathered(s, turn):
        bulk = slots[s].at[turn, pl.ds(0, flows[s][2] - 1), :]
        return pltpu.make_async_remote_copy(
            src_ref=bulk, dst_ref=bulk, send_sem=red_send[s].at[turn], recv_sem=red_recv[s].at[turn],
            device_id={"level": 1 - level, "gx": gx, "yz": yz}, device_id_type=MESH)

    def reduce_all(accs, turn, meanwhile):
        n = len(accs)
        size = -(-n // 8) * 8
        eye = lax.broadcasted_iota(jnp.int32, (size, LANES), 0) == lax.broadcasted_iota(jnp.int32, (size, LANES), 1)
        tall = jnp.concatenate([jnp.sum(a, axis=0, keepdims=True) for a in accs]
                               + [jnp.zeros((size - n, LANES), jnp.float32)] * (size > n), axis=0)
        col = jnp.sum(tall, axis=1, keepdims=True)
        line = jnp.sum(jnp.where(eye, col, 0.0), axis=0, keepdims=True)
        for s in range(len(flows)):
            slots[s][turn, pl.ds(flows[s][1], 1), :] = line

            def start(s=s):
                for copy in cast(s, turn):
                    copy.start()

            def finish(s=s):
                gathered(s, turn).wait_recv()

            last = s == len(flows) - 1
            alone = last and turn == STEPS
            pl.when(level == 1)(start) if alone else start()
            if s == 0 and turn == 0:
                meet(ROUNDS)
            if last:
                meanwhile()
            pl.when(level == 1)(finish) if alone else finish()
            line = jnp.sum(slots[s][turn], axis=0, keepdims=True)
        col = jnp.sum(jnp.where(eye, line, 0.0), axis=1, keepdims=True)
        wide = jnp.broadcast_to(col, (size, LANES))
        return [jnp.broadcast_to(wide[k:k + 1, :], (8, LANES)) for k in range(n)]

    def place(part, z):
        return out_ref.at[0, pl.ds(part * half, half), :, slice(z * LANES, (z + 1) * LANES)]

    def across(z):
        return pltpu.make_async_remote_copy(
            src_ref=result.at[:, z], dst_ref=place(1, z), send_sem=p_send.at[z], recv_sem=p_recv.at[z],
            device_id={"level": 0, "gx": gx, "yz": yz}, device_id_type=MESH)

    def upward(k):
        source, target = ((own_c.at[ITERS * (STEPS % 2):ITERS * (STEPS % 2 + 1)], far_c.at[0:ITERS]), (sums.at[1], far_c.at[ITERS]))[k]
        return pltpu.make_async_remote_copy(
            src_ref=source, dst_ref=target, send_sem=up_send.at[k], recv_sem=up_recv.at[k],
            device_id={"level": 1, "gx": gx, "yz": yz}, device_id_type=MESH)

    def trade():
        @pl.when(level == 0)
        def _():
            for k in range(2):
                upward(k).start()
            for z in range(parts):
                place(0, z)[...] = result[:, z]

        @pl.when(level == 1)
        def _():
            for z in range(parts):
                across(z).start()

    for copy in loads:
        copy.wait()
    for x in range(PX, PX + half):
        for z in range(parts):
            src[x, z, PY:PY + rows, :] = src[x, z, PY:PY + rows, :] - dmp[x, z, PY:PY + rows, :] * p0[x, z, PY:PY + rows, :]
    pl.semaphore_wait(barrier, greeted)
    meet(0)
    starts = ((p0, PX, 0), (src, ITERS, 1), (dmp, ITERS - 1, 2))
    for item in starts:
        send_halo(*item)
    for turn in range(1, ROUNDS):
        meet(turn)
    for item in starts[:2]:
        wait_halo(*item)

    start, count = reach(ITERS)
    for x in range(PX - ITERS, PX + half + ITERS):
        t, centre = around(p0, x, start, count)
        ok = inside(x, start, count)
        for z in range(parts):
            r = src[x, z, pl.ds(start, count), :] - (6.0 * centre[z] - t[z])
            first[0, x, z, pl.ds(start, count), :] = jnp.where(ok, r, 0.0)
    wait_halo(*starts[2])
    accs = powers(first.at[0], (first.at[1], first.at[2], heads_p.at[0]), True)

    pending = list(starts)
    slot = len(starts)
    settle = None
    plan = []
    for turn in range(STEPS + 1):
        jobs = []
        for on, heads, at, work in ((turn < STEPS, heads_p, turn, work_p), (0 < turn < STEPS, heads_c, turn - 1, work_c)):
            if on:
                jobs.append(((heads.at[at], ITERS, slot), work))
                slot += 1
        plan.append(jobs)
    for item, _ in plan[0]:
        send_halo(*item)
    for turn in range(STEPS + 1):
        with_p, with_c = turn < STEPS, turn > 0
        jobs = plan[turn]
        now, then = ITERS * (turn % 2), ITERS * ((turn + 1) % 2)

        def meanwhile(turn=turn, jobs=jobs, settle=settle):
            if settle is not None:
                lax.fori_loop(0, half, settle, 0, unroll=2)
            if turn == STEPS:
                trade()
            for item, work in jobs:
                wait_halo(*item)
                powers(item[0], [work.at[k] for k in range(ITERS)])

        pending += [item for item, _ in jobs]
        dots = reduce_all(accs, turn, meanwhile)
        sets = [cg_coefficients(dots[6 * i:6 * i + 6]) for i in range(len(dots) // 6)]
        if with_p:
            step_p = sets[0][1]
        if with_c:
            rise_c, step_c = sets[-1]
        n_acc = 6 * ((turn + 1 < STEPS) + (turn < STEPS))

        def top(x, i, z, near, wide):
            before = heads_p[turn, x, z, wide, :]
            change = lifted(step_p, before, [work_p[k, x, z, wide, :] for k in range(ITERS)])
            fresh = []
            if turn + 1 < STEPS:
                fresh.append(before - change)
                heads_p[turn + 1, x, z, wide, :] = fresh[0]
            ground = before
            if with_c:
                ground = heads_p[0, x, z, wide, :] if turn == 1 else base[ITERS, i, z, near, :]
                ground = ground - lifted(step_c, heads_c[turn - 1, x, z, wide, :],
                                         [work_c[k, x, z, wide, :] for k in range(ITERS)])
                if turn + 1 < STEPS:
                    base[ITERS, i, z, near, :] = ground
            fresh.append(ground + 0.5 * change)
            heads_c[turn, x, z, wide, :] = fresh[-1]
            return fresh

        def lead(i, carry):
            for z in range(parts):
                for y in range(0, rows, 8):
                    top(i + PX, i, z, pl.ds(y, 8), pl.ds(PY + y, 8))
            return carry

        def update(i, accs):
            x = i + PX
            accs = list(accs)
            for z in range(parts):
                for y in range(0, rows, 8):
                    near, wide = pl.ds(y, 8), pl.ds(PY + y, 8)
                    if with_p:
                        if turn == 0:
                            v = [first[j, x, z, wide, :] for j in range(ITERS)]
                        else:
                            v = [own_p[now + j, i, z, near, :] for j in range(ITERS)]
                        v.append(heads_p[turn, x, z, wide, :])
                        v += [work_p[k, x, z, wide, :] for k in range(ITERS)]
                        change = shifted(step_p, v)
                    if with_c:
                        u = [own_c[now + j, i, z, near, :] for j in range(ITERS)]
                        u.append(heads_c[turn - 1, x, z, wide, :])
                        u += [work_c[k, x, z, wide, :] for k in range(ITERS)]
                    if turn + 1 < STEPS:
                        tops = [heads_p[turn + 1, x, z, wide, :], heads_c[turn, x, z, wide, :]]
                    else:
                        tops = top(x, i, z, near, wide)
                    news = []
                    if turn + 1 < STEPS:
                        fresh = [a - b for a, b in zip(v, change)]
                        for j in range(ITERS):
                            own_p[then + j, i, z, near, :] = fresh[j]
                        news.append(fresh)
                    if turn == 0:
                        ground = v[:ITERS]
                    else:
                        if turn == 1:
                            ground = [first[j, x, z, wide, :] for j in range(ITERS)]
                        else:
                            ground = [base[j, i, z, near, :] for j in range(ITERS)]
                        ground = [a - b for a, b in zip(ground, shifted(step_c, u))]
                        if turn + 1 < STEPS:
                            for j in range(ITERS):
                                base[j, i, z, near, :] = ground[j]
                    fresh = [a + 0.5 * b for a, b in zip(ground, change)]
                    for j in range(ITERS):
                        own_c[then + j, i, z, near, :] = fresh[j]
                    news.append(fresh)
                    news = [own + [far] for own, far in zip(news, tops)]
                    for f, fresh in enumerate(news):
                        for j in range(ITERS):
                            accs[6 * f + 2 * j] = accs[6 * f + 2 * j] + fresh[j] * fresh[j]
                            accs[6 * f + 2 * j + 1] = accs[6 * f + 2 * j + 1] + fresh[j] * fresh[j + 1]
            return tuple(accs)

        def settle(i, carry, turn=turn, now=now, rise_p=sets[0][0], rise_c=sets[-1][0]):
            x = i + PX
            for z in range(parts):
                for y in range(0, rows, 8):
                    near, wide = pl.ds(y, 8), pl.ds(PY + y, 8)
                    if turn == 0:
                        before, v = p0[x, z, wide, :], [first[j, x, z, wide, :] for j in range(ITERS)]
                    else:
                        before, v = sums[0, i, z, near, :], [own_p[now + j, i, z, near, :] for j in range(ITERS)]
                    after = before + combine(rise_p, v)
                    if turn + 1 < STEPS:
                        sums[0, i, z, near, :] = after
                    else:
                        result[i, z, near, :] = after
                    if turn > 0:
                        before = p0[x, z, wide, :] if turn == 1 else sums[1, i, z, near, :]
                        sums[1, i, z, near, :] = before + combine(
                            rise_c, [own_c[now + j, i, z, near, :] for j in range(ITERS)])
            return carry

        def last(i, carry):
            for z in range(parts):
                for y in range(0, rows, 8):
                    near, lanes = pl.ds(y, 8), slice(z * LANES, (z + 1) * LANES)
                    out_ref[0, half + i, near, lanes] = sums[1, i, z, near, :] + combine(
                        rise_c, [own_c[now + j, i, z, near, :] for j in range(ITERS)])
                    out_ref[0, i, near, lanes] = far_c[ITERS, i, z, near, :] + combine(
                        rise_c, [far_c[j, i, z, near, :] for j in range(ITERS)])
            return carry

        if turn + 1 < STEPS:
            lax.fori_loop(0, half, lead, 0, unroll=2)
            for item, _ in plan[turn + 1]:
                send_halo(*item)
        if turn < STEPS:
            accs = lax.fori_loop(0, half, update, (jnp.zeros((8, LANES), jnp.float32),) * n_acc, unroll=2)
        else:
            @pl.when(level == 1)
            def _():
                for k in range(2):
                    upward(k).wait_recv()
                lax.fori_loop(0, half, last, 0)
    for item in pending:
        end_halo(*item)
    for turn in range(STEPS + 1):
        gathered(0, turn).wait_send()
        if turn < STEPS:
            gathered(1, turn).wait_send()
        else:
            pl.when(level == 1)(lambda turn=turn: gathered(1, turn).wait_send())
    for z in range(parts):
        pl.when(level == 1)(lambda z=z: across(z).wait_send())
        pl.when(level == 0)(lambda z=z: across(z).wait_recv())
    for k in range(2):
        pl.when(level == 0)(lambda k=k: upward(k).wait_send())


def solution(mesh):
    levels, nx, ny = mesh.shape["level"], mesh.shape["gx"], mesh.shape["yz"]

    def per_device(init_field, source, damping):
        deep, rows, wide = init_field.shape
        half, parts = deep // levels, wide // LANES
        padded = (half + 2 * PX, parts, rows + 2 * PY, LANES)
        plain = (half, parts, rows, LANES)
        counts = (levels, nx * ny)
        turns = STEPS + 1
        dma = pltpu.SemaphoreType.DMA
        exchanges = 3 + 2 * STEPS - 1
        vmem = lambda n, shape: pltpu.VMEM((n,) + shape, jnp.float32)
        return pl.pallas_call(
            functools.partial(body, (levels, nx, ny)),
            out_shape=pltpu.VMEM((1, deep, rows, wide), jnp.float32),
            in_specs=[pl.BlockSpec(memory_space=pltpu.HBM)] * 3,
            out_specs=pl.BlockSpec(memory_space=pltpu.VMEM),
            scratch_shapes=[
                pltpu.VMEM(padded, jnp.float32),
                pltpu.VMEM(padded, jnp.float32),
                pltpu.VMEM(padded, jnp.float32),
                vmem(ITERS, padded),
                vmem(STEPS, padded),
                vmem(STEPS, padded),
                vmem(2 * ITERS, plain),
                vmem(2 * ITERS, plain),
                vmem(ITERS + 1, plain),
                vmem(ITERS, padded),
                vmem(ITERS, padded),
                vmem(2, plain),
                pltpu.VMEM(plain, jnp.float32),
                vmem(ITERS + 1, plain),
                [pltpu.VMEM((turns, n, LANES), jnp.float32) for n in counts],
                dma((3, parts)),
                dma((exchanges, 8)),
                dma((exchanges, 8)),
                [dma((turns,)) for n in counts],
                [dma((turns,)) for n in counts],
                dma((parts,)),
                dma((parts,)),
                dma((2,)),
                dma((2,)),
                pltpu.SemaphoreType.REGULAR((ROUNDS,)),
            ],
            compiler_params=pltpu.CompilerParams(has_side_effects=True, collective_id=0),
        )(init_field, source, damping)

    spec = P("gx", "yz", None)
    return jax.shard_map(
        per_device, mesh=mesh, in_specs=(spec, spec, spec),
        out_specs=P("level", "gx", "yz", None), check_vma=False,
    )
```

```python
import functools

import jax
import jax.numpy as jnp
from jax import lax
from jax.experimental import pallas as pl
from jax.experimental.pallas import tpu as pltpu
from jax.sharding import PartitionSpec as P

STEPS = 3
ITERS = 3
ROUNDS = 3
INNER = 4
PX = 4
PY = 8
LANES = 128
MID = 8.025
HALF = 6.975
MESH = pl.DeviceIdType.MESH
DIRS = ((-1, 0), (1, 0), (0, -1), (0, 1), (-1, -1), (-1, 1), (1, -1), (1, 1))


def times_a(c):
    out = [MID * v for v in c] + [jnp.zeros_like(c[0])]
    for k, v in enumerate(c):
        if k == 0:
            out[1] = out[1] + HALF * v
        else:
            out[k + 1] = out[k + 1] + (0.5 * HALF) * v
            out[k - 1] = out[k - 1] + (0.5 * HALF) * v
    return out


def plus(a, b):
    short, long = (a, b) if len(a) < len(b) else (b, a)
    return [x + y for x, y in zip(short, long)] + long[len(short):]


def scaled(s, a):
    return [s * x for x in a]


def cg_coefficients(dots):
    m = [dots[0], dots[1], 2.0 * dots[2] - dots[0], 2.0 * dots[3] - dots[1],
         2.0 * dots[4] - dots[0], 2.0 * dots[5] - dots[1]]

    def inner(a, b):
        total = None
        for i, x in enumerate(a):
            for j, y in enumerate(b):
                term = (x * y) * (0.5 * (m[i + j] + m[abs(i - j)]))
                total = term if total is None else total + term
        return total

    one = jnp.ones_like(m[0])
    resid = [one]
    direction = resid
    image = times_a(resid)
    along = image
    norm_now = m[0]
    alpha = norm_now / inner(resid, image)
    answer = None
    for step in range(ITERS):
        move = scaled(alpha, direction)
        answer = move if answer is None else plus(answer, move)
        if step + 1 < ITERS:
            resid = plus(resid, scaled(-alpha, along))
            image = times_a(resid)
            norm_next = inner(resid, resid)
            product = inner(resid, image)
            ratio = norm_next / norm_now
            alpha = norm_next / (product - ratio * norm_next / alpha)
            direction = plus(resid, scaled(ratio, direction))
            along = plus(image, scaled(ratio, along))
            norm_now = norm_next
    change = plus(times_a(answer), scaled(-1.0, answer))
    return answer, change


def shifted(c, v):
    t, w = v[:ITERS + 1], v[ITERS + 1:]
    one, two = 0.5 * c[1], 0.5 * c[2]
    even, odd, gap = t[0] + t[2], t[1] + t[3], t[0] - t[2]
    return [
        c[0] * t[0] + c[1] * t[1] + (c[2] * t[2] + c[3] * t[3]),
        c[0] * t[1] + one * even + (two * odd + c[3] * w[0]),
        c[0] * t[2] + one * odd + (two * gap + c[2] * w[0]) + c[3] * w[1],
    ]


def lifted(c, t, w):
    return c[0] * t + c[1] * w[0] + (c[2] * w[1] + c[3] * w[2])


def combine(c, v):
    total = None
    for a, b in zip(c, v):
        total = a * b if total is None else total + a * b
    return total


def body(sizes, init_ref, source_ref, damp_ref, out_ref, p0, src, dmp, first, heads_p, heads_c, own_p, own_c,
         base, work_p, work_c, sums, result, far_c, slots, in_sem, send_sem, recv_sem, red_send, red_recv, p_send, p_recv, up_send, up_recv,
         met):
    levels, nx, ny = sizes
    half = own_p.shape[1]
    parts = p0.shape[1]
    rows = own_p.shape[3]
    level, gx, yz = lax.axis_index("level"), lax.axis_index("gx"), lax.axis_index("yz")
    xpos = gx * levels + level
    xcount = nx * levels
    x_in = (xpos > 0, xpos < xcount - 1)
    y_in = (yz > 0, yz < ny - 1)

    def exists(dx, dy):
        ok = None
        for d, at, count in ((dx, xpos, xcount), (dy, yz, ny)):
            if d != 0:
                c = at + d >= 0 if d < 0 else at + d < count
                ok = c if ok is None else jnp.logical_and(ok, c)
        return ok

    def beside(dx, dy):
        to = xpos + dx
        return {"level": lax.rem(to + xcount, levels), "gx": lax.div(to + xcount, levels) - nx, "yz": yz + dy}

    mine = pl.ds(level * half, half)
    loads = []
    for i, (ref, buf) in enumerate(((init_ref, p0), (source_ref, src), (damp_ref, dmp))):
        for z in range(parts):
            copy = pltpu.make_async_copy(ref.at[mine, :, slice(z * LANES, (z + 1) * LANES)],
                                         buf.at[PX:PX + half, z, PY:PY + rows, :], in_sem.at[i, z])
            copy.start()
            loads.append(copy)

    def signal_all(sem, steps):
        count = 0
        for dx, dy in steps:
            ok = exists(dx, dy)
            count = count + jnp.where(ok, 1, 0)

            @pl.when(ok)
            def _(dx=dx, dy=dy):
                pl.semaphore_signal(sem, inc=1, device_id=beside(dx, dy), device_id_type=MESH)
        return count

    inner = INNER if ny % INNER == 0 else 1
    extent = {"level": levels, "gx": nx, "outer": ny // inner, "inner": inner}
    here = {"level": level, "gx": gx, "outer": lax.div(yz, inner), "inner": lax.rem(yz, inner)}
    ring = {a: [here[a]] + [lax.rem(here[a] + off, n) for off in range(1, n)] for a, n in extent.items()}
    deep = extent["outer"]
    rounds = ([(0, k) for k in range(1, inner)] + [(1, 0), (deep - 1, 0)],
              [(1, 0), (2, 0), (deep - 2, 0), (deep - 1, 0)],
              [(k, 0) for k in range(3, deep - 2)])

    def call(sem, steps):
        for far, near in steps:
            pl.semaphore_signal(sem, inc=1, device_id_type=MESH, device_id={
                "level": level, "gx": gx, "yz": ring["outer"][far] * inner + ring["inner"][near]})

    def meet(turn):
        if turn > 0:
            pl.semaphore_wait(met.at[turn - 1], len(rounds[turn - 1]))
        if turn < ROUNDS:
            call(met.at[turn], rounds[turn])

    barrier = pltpu.get_barrier_semaphore()
    greeted = signal_all(barrier, DIRS + tuple((d, 0) for d in range(1 - xcount, xcount) if abs(d) > 1)) + len(rounds[0])
    call(barrier, rounds[0])

    zero_x = jnp.zeros((PX,) + tuple(p0.shape[1:]), jnp.float32)
    zero_y = jnp.zeros((p0.shape[0], parts, PY, LANES), jnp.float32)
    for buf in [p0] + [heads_p.at[n] for n in range(STEPS)] + [heads_c.at[n] for n in range(STEPS - 1)]:
        @pl.when(jnp.logical_not(x_in[0]))
        def _(buf=buf):
            buf[0:PX] = zero_x

        @pl.when(jnp.logical_not(x_in[1]))
        def _(buf=buf):
            buf[PX + half:] = zero_x

        @pl.when(jnp.logical_not(y_in[0]))
        def _(buf=buf):
            buf[:, :, 0:PY, :] = zero_y

        @pl.when(jnp.logical_not(y_in[1]))
        def _(buf=buf):
            buf[:, :, PY + rows:, :] = zero_y

    def halo_copy(buf, width, slot, k):
        dx, dy = DIRS[k]
        w = width if 0 in (dx, dy) else width - 1

        def spans(d, pad, size):
            if d == 0:
                return slice(pad, pad + size), slice(pad, pad + size)
            if d < 0:
                return slice(pad, pad + w), slice(pad + size, pad + size + w)
            return slice(pad + size - w, pad + size), slice(pad - w, pad)

        sx, tx = spans(dx, PX, half)
        sy, ty = spans(dy, PY, rows)
        return pltpu.make_async_remote_copy(
            src_ref=buf.at[sx, :, sy, :], dst_ref=buf.at[tx, :, ty, :],
            send_sem=send_sem.at[slot, k], recv_sem=recv_sem.at[slot, k],
            device_id=beside(dx, dy), device_id_type=MESH,
        )

    order = (2, 3, 4, 5, 6, 7, 0, 1)

    def send_halo(*item):
        for k in order:
            pl.when(exists(*DIRS[k]))(lambda k=k: halo_copy(*item, k).start())

    def wait_halo(*item):
        for k in order:
            dx, dy = DIRS[k]
            pl.when(exists(-dx, -dy))(lambda k=k: halo_copy(*item, k).wait_recv())

    def end_halo(*item):
        for k in order:
            pl.when(exists(*DIRS[k]))(lambda k=k: halo_copy(*item, k).wait_send())

    def around(v, x, start, count):
        lane = lax.broadcasted_iota(jnp.int32, (count, LANES), 1)
        own = pl.ds(start, count)
        centre = [v[x, z, own, :] for z in range(parts)]
        fore = [pltpu.roll(c, 1, 1) for c in centre]
        back = [pltpu.roll(c, LANES - 1, 1) for c in centre]
        out = []
        for z in range(parts):
            near = jnp.where(lane == 0, fore[z - 1] if z > 0 else 0.0, fore[z])
            far = jnp.where(lane == LANES - 1, back[z + 1] if z + 1 < parts else 0.0, back[z])
            beside = v[x - 1, z, own, :] + v[x + 1, z, own, :]
            beside = beside + v[x, z, pl.ds(start - 1, count), :] + v[x, z, pl.ds(start + 1, count), :]
            beside = beside + (near + far)
            out.append(beside)
        return out, centre

    def stencil(v, x, start, count):
        out, centre = around(v, x, start, count)
        own = pl.ds(start, count)
        return [(dmp[x, z, own, :] + (7.0 - MID)) * centre[z] - out[z] for z in range(parts)], centre

    low = jnp.where(y_in[0], 0, PY)
    high = jnp.where(y_in[1], 2 * PY + rows, PY + rows)

    def fold(block):
        return jnp.sum(block.reshape(-1, 8, LANES), axis=0)

    def reach(h):
        return PY - h, -(-(rows + 2 * h) // 8) * 8

    def inside(x, start, count):
        row = lax.broadcasted_iota(jnp.int32, (count, LANES), 0) + start
        ok = jnp.logical_and(row >= low, row < high)
        if PX <= x < PX + half:
            return ok
        return jnp.logical_and(ok, x_in[0] if x < PX else x_in[1])

    def powers(head, work, with_dots=False):
        zero = jnp.zeros((8, LANES), jnp.float32)
        totals = []
        for k in range(1, ITERS + 1):
            h = ITERS - k
            start, count = reach(h)
            prev = head if k == 1 else work[k - 2]
            older = None if k == 1 else head if k == 2 else work[k - 3]
            row = lax.broadcasted_iota(jnp.int32, (count, LANES), 0) + start
            keep = jnp.logical_and(row >= PY, row < PY + rows)
            a, b = zero, zero
            for x in range(PX - h, PX + half + h):
                t, centre = stencil(prev, x, start, count)
                ok = inside(x, start, count)
                for z in range(parts):
                    if k == 1:
                        new = t[z] * (1.0 / HALF)
                    else:
                        new = t[z] * (2.0 / HALF) - older[x, z, pl.ds(start, count), :]
                    if h > 0:
                        new = jnp.where(ok, new, 0.0)
                    work[k - 1][x, z, pl.ds(start, count), :] = new
                    if with_dots and PX <= x < PX + half:
                        square, cross = centre[z] * centre[z], centre[z] * new
                        if h > 0:
                            square, cross = jnp.where(keep, square, 0.0), jnp.where(keep, cross, 0.0)
                        a = a + fold(square)
                        b = b + fold(cross)
            totals += [a, b]
        return totals

    flows = []
    for axes in (("level",), ("gx", "outer", "inner")):
        peers, me, n = [{}], 0, 1
        for a in axes:
            peers = [dict(p, **{a: off}) for p in peers for off in range(extent[a])]
            me, n = me * extent[a] + here[a], n * extent[a]
        peers = [p for p in peers if any(p.values())]
        peers.sort(key=lambda p: -sum(min(off, extent[a] - off) for a, off in p.items()))
        flows.append((peers, me, n))

    def cast(s, turn):
        peers, me, n = flows[s]
        copies = []
        for p in peers:
            at = {a: ring[a][p.get(a, 0)] for a in extent}
            cell = slots[s].at[turn, pl.ds(me, 1), :]
            copies.append(pltpu.make_async_remote_copy(
                src_ref=cell, dst_ref=cell, send_sem=red_send[s].at[turn], recv_sem=red_recv[s].at[turn],
                device_id={"level": at["level"], "gx": at["gx"], "yz": at["outer"] * inner + at["inner"]}, device_id_type=MESH))
        return copies

    def gathered(s, turn):
        bulk = slots[s].at[turn, pl.ds(0, flows[s][2] - 1), :]
        return pltpu.make_async_remote_copy(
            src_ref=bulk, dst_ref=bulk, send_sem=red_send[s].at[turn], recv_sem=red_recv[s].at[turn],
            device_id={"level": 1 - level, "gx": gx, "yz": yz}, device_id_type=MESH)

    def reduce_all(accs, turn, meanwhile):
        n = len(accs)
        size = -(-n // 8) * 8
        eye = lax.broadcasted_iota(jnp.int32, (size, LANES), 0) == lax.broadcasted_iota(jnp.int32, (size, LANES), 1)
        tall = jnp.concatenate([jnp.sum(a, axis=0, keepdims=True) for a in accs]
                               + [jnp.zeros((size - n, LANES), jnp.float32)] * (size > n), axis=0)
        col = jnp.sum(tall, axis=1, keepdims=True)
        line = jnp.sum(jnp.where(eye, col, 0.0), axis=0, keepdims=True)
        for s in range(len(flows)):
            slots[s][turn, pl.ds(flows[s][1], 1), :] = line

            def start(s=s):
                for copy in cast(s, turn):
                    copy.start()

            def finish(s=s):
                gathered(s, turn).wait_recv()

            last = s == len(flows) - 1
            alone = last and turn == STEPS
            pl.when(level == 1)(start) if alone else start()
            if s == 0 and turn == 0:
                meet(ROUNDS)
            if last:
                meanwhile()
            pl.when(level == 1)(finish) if alone else finish()
            line = jnp.sum(slots[s][turn], axis=0, keepdims=True)
        col = jnp.sum(jnp.where(eye, line, 0.0), axis=1, keepdims=True)
        wide = jnp.broadcast_to(col, (size, LANES))
        return [jnp.broadcast_to(wide[k:k + 1, :], (8, LANES)) for k in range(n)]

    def place(part, z):
        return out_ref.at[0, pl.ds(part * half, half), :, slice(z * LANES, (z + 1) * LANES)]

    def across(z):
        return pltpu.make_async_remote_copy(
            src_ref=result.at[:, z], dst_ref=place(1, z), send_sem=p_send.at[z], recv_sem=p_recv.at[z],
            device_id={"level": 0, "gx": gx, "yz": yz}, device_id_type=MESH)

    def upward(k):
        source, target = ((own_c.at[ITERS * (STEPS % 2):ITERS * (STEPS % 2 + 1)], far_c.at[0:ITERS]), (sums.at[1], far_c.at[ITERS]))[k]
        return pltpu.make_async_remote_copy(
            src_ref=source, dst_ref=target, send_sem=up_send.at[k], recv_sem=up_recv.at[k],
            device_id={"level": 1, "gx": gx, "yz": yz}, device_id_type=MESH)

    def trade():
        @pl.when(level == 0)
        def _():
            for k in range(2):
                upward(k).start()
            for z in range(parts):
                place(0, z)[...] = result[:, z]

        @pl.when(level == 1)
        def _():
            for z in range(parts):
                across(z).start()

    for copy in loads:
        copy.wait()
    for x in range(PX, PX + half):
        for z in range(parts):
            src[x, z, PY:PY + rows, :] = src[x, z, PY:PY + rows, :] - dmp[x, z, PY:PY + rows, :] * p0[x, z, PY:PY + rows, :]
    pl.semaphore_wait(barrier, greeted)
    meet(0)
    starts = ((p0, PX, 0), (src, ITERS, 1), (dmp, ITERS - 1, 2))
    for item in starts:
        send_halo(*item)
    for turn in range(1, ROUNDS):
        meet(turn)
    for item in starts[:2]:
        wait_halo(*item)

    start, count = reach(ITERS)
    for x in range(PX - ITERS, PX + half + ITERS):
        t, centre = around(p0, x, start, count)
        ok = inside(x, start, count)
        for z in range(parts):
            r = src[x, z, pl.ds(start, count), :] - (6.0 * centre[z] - t[z])
            first[0, x, z, pl.ds(start, count), :] = jnp.where(ok, r, 0.0)
    wait_halo(*starts[2])
    accs = powers(first.at[0], (first.at[1], first.at[2], heads_p.at[0]), True)

    pending = list(starts)
    slot = len(starts)
    settle = None
    plan = []
    for turn in range(STEPS + 1):
        jobs = []
        for on, heads, at, work in ((turn < STEPS, heads_p, turn, work_p), (0 < turn < STEPS, heads_c, turn - 1, work_c)):
            if on:
                jobs.append(((heads.at[at], ITERS, slot), work))
                slot += 1
        plan.append(jobs)
    for item, _ in plan[0]:
        send_halo(*item)
    for turn in range(STEPS + 1):
        with_p, with_c = turn < STEPS, turn > 0
        jobs = plan[turn]
        now, then = ITERS * (turn % 2), ITERS * ((turn + 1) % 2)

        def meanwhile(turn=turn, jobs=jobs, settle=settle):
            if settle is not None:
                lax.fori_loop(0, half, settle, 0, unroll=2)
            if turn == STEPS:
                trade()
            for item, work in jobs:
                wait_halo(*item)
                powers(item[0], [work.at[k] for k in range(ITERS)])

        pending += [item for item, _ in jobs]
        dots = reduce_all(accs, turn, meanwhile)
        sets = [cg_coefficients(dots[6 * i:6 * i + 6]) for i in range(len(dots) // 6)]
        if with_p:
            step_p = sets[0][1]
        if with_c:
            rise_c, step_c = sets[-1]
        n_acc = 6 * ((turn + 1 < STEPS) + (turn < STEPS))

        def top(x, i, z, near, wide):
            before = heads_p[turn, x, z, wide, :]
            change = lifted(step_p, before, [work_p[k, x, z, wide, :] for k in range(ITERS)])
            fresh = []
            if turn + 1 < STEPS:
                fresh.append(before - change)
                heads_p[turn + 1, x, z, wide, :] = fresh[0]
            ground = before
            if with_c:
                ground = heads_p[0, x, z, wide, :] if turn == 1 else base[ITERS, i, z, near, :]
                ground = ground - lifted(step_c, heads_c[turn - 1, x, z, wide, :],
                                         [work_c[k, x, z, wide, :] for k in range(ITERS)])
                if turn + 1 < STEPS:
                    base[ITERS, i, z, near, :] = ground
            fresh.append(ground + 0.5 * change)
            heads_c[turn, x, z, wide, :] = fresh[-1]
            return fresh

        def lead(i, carry):
            for z in range(parts):
                for y in range(0, rows, 8):
                    top(i + PX, i, z, pl.ds(y, 8), pl.ds(PY + y, 8))
            return carry

        def update(i, accs):
            x = i + PX
            accs = list(accs)
            for z in range(parts):
                for y in range(0, rows, 8):
                    near, wide = pl.ds(y, 8), pl.ds(PY + y, 8)
                    if with_p:
                        if turn == 0:
                            v = [first[j, x, z, wide, :] for j in range(ITERS)]
                        else:
                            v = [own_p[now + j, i, z, near, :] for j in range(ITERS)]
                        v.append(heads_p[turn, x, z, wide, :])
                        v += [work_p[k, x, z, wide, :] for k in range(ITERS)]
                        change = shifted(step_p, v)
                    if with_c:
                        u = [own_c[now + j, i, z, near, :] for j in range(ITERS)]
                        u.append(heads_c[turn - 1, x, z, wide, :])
                        u += [work_c[k, x, z, wide, :] for k in range(ITERS)]
                    if turn + 1 < STEPS:
                        tops = [heads_p[turn + 1, x, z, wide, :], heads_c[turn, x, z, wide, :]]
                    else:
                        tops = top(x, i, z, near, wide)
                    news = []
                    if turn + 1 < STEPS:
                        fresh = [a - b for a, b in zip(v, change)]
                        for j in range(ITERS):
                            own_p[then + j, i, z, near, :] = fresh[j]
                        news.append(fresh)
                    if turn == 0:
                        ground = v[:ITERS]
                    else:
                        if turn == 1:
                            ground = [first[j, x, z, wide, :] for j in range(ITERS)]
                        else:
                            ground = [base[j, i, z, near, :] for j in range(ITERS)]
                        ground = [a - b for a, b in zip(ground, shifted(step_c, u))]
                        if turn + 1 < STEPS:
                            for j in range(ITERS):
                                base[j, i, z, near, :] = ground[j]
                    fresh = [a + 0.5 * b for a, b in zip(ground, change)]
                    for j in range(ITERS):
                        own_c[then + j, i, z, near, :] = fresh[j]
                    news.append(fresh)
                    news = [own + [far] for own, far in zip(news, tops)]
                    for f, fresh in enumerate(news):
                        for j in range(ITERS):
                            accs[6 * f + 2 * j] = accs[6 * f + 2 * j] + fresh[j] * fresh[j]
                            accs[6 * f + 2 * j + 1] = accs[6 * f + 2 * j + 1] + fresh[j] * fresh[j + 1]
            return tuple(accs)

        def settle(i, carry, turn=turn, now=now, rise_p=sets[0][0], rise_c=sets[-1][0]):
            x = i + PX
            for z in range(parts):
                for y in range(0, rows, 8):
                    near, wide = pl.ds(y, 8), pl.ds(PY + y, 8)
                    if turn == 0:
                        before, v = p0[x, z, wide, :], [first[j, x, z, wide, :] for j in range(ITERS)]
                    else:
                        before, v = sums[0, i, z, near, :], [own_p[now + j, i, z, near, :] for j in range(ITERS)]
                    after = before + combine(rise_p, v)
                    if turn + 1 < STEPS:
                        sums[0, i, z, near, :] = after
                    else:
                        result[i, z, near, :] = after
                    if turn > 0:
                        before = p0[x, z, wide, :] if turn == 1 else sums[1, i, z, near, :]
                        sums[1, i, z, near, :] = before + combine(
                            rise_c, [own_c[now + j, i, z, near, :] for j in range(ITERS)])
            return carry

        def last(i, carry):
            for z in range(parts):
                for y in range(0, rows, 8):
                    near, lanes = pl.ds(y, 8), slice(z * LANES, (z + 1) * LANES)
                    out_ref[0, half + i, near, lanes] = sums[1, i, z, near, :] + combine(
                        rise_c, [own_c[now + j, i, z, near, :] for j in range(ITERS)])
                    out_ref[0, i, near, lanes] = far_c[ITERS, i, z, near, :] + combine(
                        rise_c, [far_c[j, i, z, near, :] for j in range(ITERS)])
            return carry

        if turn + 1 < STEPS:
            lax.fori_loop(0, half, lead, 0, unroll=2)
            for item, _ in plan[turn + 1]:
                send_halo(*item)
        if turn < STEPS:
            accs = lax.fori_loop(0, half, update, (jnp.zeros((8, LANES), jnp.float32),) * n_acc, unroll=2)
        else:
            @pl.when(level == 1)
            def _():
                for k in range(2):
                    upward(k).wait_recv()
                lax.fori_loop(0, half, last, 0, unroll=4)
    for item in pending:
        end_halo(*item)
    for turn in range(STEPS + 1):
        gathered(0, turn).wait_send()
        if turn < STEPS:
            gathered(1, turn).wait_send()
        else:
            pl.when(level == 1)(lambda turn=turn: gathered(1, turn).wait_send())
    for z in range(parts):
        pl.when(level == 1)(lambda z=z: across(z).wait_send())
        pl.when(level == 0)(lambda z=z: across(z).wait_recv())
    for k in range(2):
        pl.when(level == 0)(lambda k=k: upward(k).wait_send())


def solution(mesh):
    levels, nx, ny = mesh.shape["level"], mesh.shape["gx"], mesh.shape["yz"]

    def per_device(init_field, source, damping):
        deep, rows, wide = init_field.shape
        half, parts = deep // levels, wide // LANES
        padded = (half + 2 * PX, parts, rows + 2 * PY, LANES)
        plain = (half, parts, rows, LANES)
        counts = (levels, nx * ny)
        turns = STEPS + 1
        dma = pltpu.SemaphoreType.DMA
        exchanges = 3 + 2 * STEPS - 1
        vmem = lambda n, shape: pltpu.VMEM((n,) + shape, jnp.float32)
        return pl.pallas_call(
            functools.partial(body, (levels, nx, ny)),
            out_shape=pltpu.VMEM((1, deep, rows, wide), jnp.float32),
            in_specs=[pl.BlockSpec(memory_space=pltpu.HBM)] * 3,
            out_specs=pl.BlockSpec(memory_space=pltpu.VMEM),
            scratch_shapes=[
                pltpu.VMEM(padded, jnp.float32),
                pltpu.VMEM(padded, jnp.float32),
                pltpu.VMEM(padded, jnp.float32),
                vmem(ITERS, padded),
                vmem(STEPS, padded),
                vmem(STEPS, padded),
                vmem(2 * ITERS, plain),
                vmem(2 * ITERS, plain),
                vmem(ITERS + 1, plain),
                vmem(ITERS, padded),
                vmem(ITERS, padded),
                vmem(2, plain),
                pltpu.VMEM(plain, jnp.float32),
                vmem(ITERS + 1, plain),
                [pltpu.VMEM((turns, n, LANES), jnp.float32) for n in counts],
                dma((3, parts)),
                dma((exchanges, 8)),
                dma((exchanges, 8)),
                [dma((turns,)) for n in counts],
                [dma((turns,)) for n in counts],
                dma((parts,)),
                dma((parts,)),
                dma((2,)),
                dma((2,)),
                pltpu.SemaphoreType.REGULAR((ROUNDS,)),
            ],
            compiler_params=pltpu.CompilerParams(has_side_effects=True, collective_id=0),
        )(init_field, source, damping)

    spec = P("gx", "yz", None)
    return jax.shard_map(
        per_device, mesh=mesh, in_specs=(spec, spec, spec),
        out_specs=P("level", "gx", "yz", None), check_vma=False,
    )
```
